128 devices in a mesh: dp: 2 (over x_lo), expert: 32 (over y, z, core), tensor: 2 (over x_hi).
Axes of the slice: x: 4 (x_hi: 2, x_lo: 2; x = x_hi * 2 + x_lo), y: 4, z: 4, core: 2. Of those that a mesh axis runs over, the one named last changes fastest.
Arguments:
- tokens: bfloat16 [8192, 2048], P(('dp', 'expert')), may hold values from -6 to 6
- norm_gain: float32 [2048], replicated, may hold values from 0.1 to 1.9
- router: bfloat16 [2048, 32], replicated, may hold values from -0.125 to 0.125
- expert_ids: int32 [8192, 4], P(('dp', 'expert')), may hold values from 0 to 31, all different within a row; in each aligned block of 128 rows (0 to 127, 128 to 255, ...) at most 20 rows name the same one
- modality: int32 [8192], P(('dp', 'expert')), may hold values from 0 to 1, as said below
- expert_gate: bfloat16 [32, 2048, 1408], P('expert', None, 'tensor'), may hold values from -0.125 to 0.125
- expert_up: bfloat16 [32, 2048, 1408], P('expert', None, 'tensor'), may hold values from -0.125 to 0.125
- expert_down: bfloat16 [32, 1408, 2048], P('expert', 'tensor'), may hold values from -0.15625 to 0.15625
- shared_gate: bfloat16 [2, 2048, 704], P(None, None, ('dp', 'tensor')), may hold values from -0.125 to 0.125
- shared_up: bfloat16 [2, 2048, 704], P(None, None, ('dp', 'tensor')), may hold values from -0.125 to 0.125
- shared_down: bfloat16 [2, 704, 2048], P(None, ('dp', 'tensor')), may hold values from -0.21875 to 0.21875
Outputs:
- mixed: bfloat16 [8192, 2048], P(('dp', 'expert'), 'tensor')
The draws below stay inside these ranges and needn't reach their ends.
Inputs may be any that keep to these rules, and one draw needn't show every extreme that they name: `expert_ids`: each token names 4 different experts; among the 128 tokens of one device (aligned blocks of rows) no expert is named by more than 20 tokens, and some expert reaches 20. `modality`: within each aligned block of 128 tokens the image patches form one run (taken cyclically) that covers from an eighth to seven eighths of the block.
All inputs are finite; a program needn't handle non-finite values.
Results may differ from the reference program's by a relative error of at most 0.0073.
Values may be sent and summed in bfloat16 or wider, within the bound.
No kernel may reach another device: no remote copies, remote signals or barrier semaphores. Data moves between devices by JAX's collectives and lax.ppermute only.
A program may use at most 128 MiB of HBM per device.

```python
import math
import jax
import jax.numpy as jnp
import numpy as np
from jax import lax

D = 2048
FF = 1408
SH = 704
TOP = 4
TOK_DEV = 128
EXPERTS = 32
TOKENS = 8192
CAP = 20


def draw_modality(key, part):
    blocks = TOKENS // TOK_DEV
    share_key, start_key = jax.random.split(jax.random.fold_in(key, 11))
    counts = jax.random.randint(share_key, (blocks, 1), TOK_DEV // 8, TOK_DEV - TOK_DEV // 8 + 1)
    starts = jax.random.randint(start_key, (blocks, 1), 0, TOK_DEV)
    position = jnp.arange(TOK_DEV, dtype=jnp.int32)[None, :]
    image_flags = ((position - starts) % TOK_DEV < counts).astype(jnp.int32)
    return image_flags.reshape(-1)


def steps_of(stream_key, shape, pieces, smallest, high):
    loudness, own = 1.0, jax.random.fold_in(stream_key, 6)
    for dim, blocks in pieces:
        draws = jnp.exp(jax.random.uniform(jax.random.fold_in(own, dim), (blocks,), jnp.float32, smallest / len(pieces), high / len(pieces)))
        loudness = loudness * jnp.repeat(draws, shape[dim] // blocks).reshape([-1 if axis == dim else 1 for axis in range(len(shape))])
    return loudness


def deal_out(rng, own, number, rows, amount, top, bound, slope):
    ranking = jax.random.permutation(rng, amount)
    heavy_load, usual = portions_of(amount, rows * top, bound, slope, True), portions_of(amount, rows * top, bound, slope, False)
    places = jnp.arange(amount)

    def named(tallies, rotation):
        used = int((tallies > 0).sum())
        fixed = max(1, used // 4)
        passed = fixed + (places - fixed + rotation * (used - fixed)) % max(1, amount - fixed)
        return jnp.zeros((amount,), jnp.int32).at[ranking[jnp.where(places < fixed, places, passed)]].set(jnp.asarray(tallies, jnp.int32))

    tallies = jnp.where(number % 4 == 0, named(heavy_load, number // 4), named(usual, number - number // 4 - 1))
    mixed = jax.random.permutation(jax.random.fold_in(own, 3), amount)
    giver, sink = mixed[0:amount // 2 * 2:2], mixed[1:amount // 2 * 2:2]
    margin = jnp.minimum(tallies[giver] - 1, bound - tallies[sink]) // 2
    margin = jnp.where((giver == ranking[0]) | (sink == ranking[0]) | (tallies[sink] == 0), 0, jnp.maximum(margin, 0))
    passed = jax.random.randint(jax.random.fold_in(own, 4), (amount // 2,), 0, 1 << 20) % (margin + 1)
    tallies = tallies.at[giver].add(-passed).at[sink].add(passed)
    labels = jnp.searchsorted(jnp.cumsum(tallies), jnp.arange(rows * top), side="right").astype(jnp.int32)
    listing = labels.reshape(top, rows).T
    listing = listing[jax.random.permutation(jax.random.fold_in(own, 1), rows)]
    rotation = jax.random.randint(jax.random.fold_in(own, 2), (rows, 1), 0, top)
    return jnp.take_along_axis(listing, (jnp.arange(top)[None, :] + rotation) % top, axis=1)


def portions_of(amount, total, reach, skew, full):
    weights = [(1 << 20) // math.isqrt(rank ** skew) + 1 for rank in range(1, amount + 1)]
    largest = reach if full else min(reach, max(-(-total // amount), total * weights[0] // sum(weights)))
    least = 1 if total - largest >= amount - 1 else 0
    given, spare = [largest] + [least] * (amount - 1), total - largest - least * (amount - 1)
    while spare > 0:
        free = [i for i in range(1, amount) if given[i] < largest] or [i for i in range(1, amount) if given[i] < reach]
        whole, left = sum([weights[i] for i in free]), spare
        for i in free:
            addition = min(reach - given[i], max(1, left * weights[i] // whole), spare)
            given[i] = given[i] + addition
            spare = spare - addition
    return np.array(given)


def bell_draw(rng, dims, scale, limit, pieces=(), held_as=jnp.bfloat16):
    array = scale * jax.random.normal(rng, dims, jnp.float32)
    if pieces:
        array = array * steps_of(rng, dims, pieces, -0.22, 0.18)
    return jnp.clip(array, -limit, limit).astype(held_as)


def setup_inputs(seed: int = 0) -> dict:
    key_list = jax.random.split(jax.random.key(seed), 12)
    tokens = bell_draw(key_list[0], (TOKENS, D), 1.0, 6.0, ((0, 64),))
    norm_gain = jnp.clip(1.0 + 0.18 * jax.random.normal(key_list[1], (D,), jnp.float32), 0.1, 1.9)
    router = bell_draw(key_list[2], (D, EXPERTS), D ** -0.5, 0.125)
    expert_ids_keys = jax.random.split(jax.random.fold_in(key_list[3], 1), TOKENS // TOK_DEV)
    expert_ids_turns = jax.random.permutation(jax.random.fold_in(key_list[3], 3), TOKENS // TOK_DEV)
    expert_ids = jax.vmap(lambda own, number: deal_out(jax.random.fold_in(key_list[3], 2), own, number, TOK_DEV, EXPERTS, TOP, CAP, 1))(expert_ids_keys, expert_ids_turns).reshape((TOKENS, TOP))
    modality = draw_modality(jax.random.fold_in(key_list[11], 71), 0)
    expert_gate = bell_draw(key_list[5], (EXPERTS, D, FF), D ** -0.5, 0.125, ((0, 32), (2, 2)))
    expert_up = bell_draw(key_list[6], (EXPERTS, D, FF), D ** -0.5, 0.125, ((0, 32), (2, 2)))
    expert_down = bell_draw(key_list[7], (EXPERTS, FF, D), FF ** -0.5, 0.15625, ((0, 32), (1, 2)))
    shared_gate = bell_draw(key_list[8], (2, D, SH), D ** -0.5, 0.125, ((2, 4),))
    shared_up = bell_draw(key_list[9], (2, D, SH), D ** -0.5, 0.125, ((2, 4),))
    shared_down = bell_draw(key_list[10], (2, SH, D), SH ** -0.5, 0.21875, ((1, 4),))
    return {"tokens": tokens, "norm_gain": norm_gain, "router": router, "expert_ids": expert_ids, "modality": modality, "expert_gate": expert_gate, "expert_up": expert_up, "expert_down": expert_down, "shared_gate": shared_gate, "shared_up": shared_up, "shared_down": shared_down}


epsilon = 1e-06

def rms_normed(tokens, norm_gain):
    values = tokens.astype(jnp.float32)
    inv_scale = lax.rsqrt(lax.optimization_barrier(jnp.mean(values * values, axis=-1, keepdims=True)) + epsilon)
    return (values * inv_scale * norm_gain).astype(jnp.bfloat16)

def route_weights(normed, router, expert_ids):
    logits = jnp.dot(normed, router, preferred_element_type=jnp.float32)
    chosen = jnp.take_along_axis(logits, expert_ids, axis=1)
    scores = jax.nn.sigmoid(chosen)
    return scores / lax.optimization_barrier(jnp.sum(scores, axis=1, keepdims=True))

def capacity_slots(expert_ids, expert_count, block_rows):
    row_count, top_count = expert_ids.shape
    onehot = (expert_ids[:, :, None] == jnp.arange(expert_count, dtype=jnp.int32)[None, None, :]).astype(jnp.int32)
    grouped = onehot.reshape(row_count // block_rows, block_rows * top_count, expert_count)
    running = (jnp.cumsum(grouped, axis=1, dtype=jnp.int32) - 1).reshape(row_count, top_count, expert_count)
    return lax.optimization_barrier(jnp.sum(running * onehot, axis=-1, dtype=jnp.int32)).astype(jnp.int32)

def reference(tokens, norm_gain, router, expert_ids, modality, expert_gate, expert_up, expert_down, shared_gate, shared_up, shared_down):
    normed = rms_normed(tokens, norm_gain)
    weights = route_weights(normed, router, expert_ids)
    slot_rank = capacity_slots(expert_ids, EXPERTS, TOK_DEV)
    sources = TOKENS // TOK_DEV
    token_index = jnp.broadcast_to(jnp.arange(TOKENS, dtype=jnp.int32)[:, None], (TOKENS, TOP)).astype(jnp.int32)
    source_block = (token_index // TOK_DEV).astype(jnp.int32)
    slot_table = jnp.full((EXPERTS, sources, CAP), TOKENS, jnp.int32)
    slot_table = slot_table.at[expert_ids, source_block, slot_rank].set(token_index)
    weight_table = jnp.zeros((EXPERTS, sources, CAP), jnp.float32)
    weight_table = weight_table.at[expert_ids, source_block, slot_rank].set(weights)
    padded = jnp.concatenate([normed, jnp.zeros((1, D), jnp.bfloat16)], axis=0)

    def one_expert(routed, operands):
        rows_index, slot_weight, gate_weight, up_weight, down_weight = operands
        flat_index = rows_index.reshape(-1)
        gathered = padded[flat_index]
        gate_value = jnp.dot(gathered, gate_weight, preferred_element_type=jnp.float32)
        up_value = jnp.dot(gathered, up_weight, preferred_element_type=jnp.float32)
        hidden = (jax.nn.silu(gate_value) * up_value).astype(jnp.bfloat16)
        result = jnp.dot(hidden, down_weight, preferred_element_type=jnp.float32)
        result = result * slot_weight.reshape(-1)[:, None]
        return (routed.at[flat_index].add(result), None)
    start = jnp.zeros((TOKENS + 1, D), jnp.float32)
    routed, unused = lax.scan(one_expert, start, (slot_table, weight_table, expert_gate, expert_up, expert_down))
    routed = routed[:TOKENS]

    def shared_out(modal_index):
        gate_value = jnp.dot(normed, shared_gate[modal_index], preferred_element_type=jnp.float32)
        up_value = jnp.dot(normed, shared_up[modal_index], preferred_element_type=jnp.float32)
        hidden = (jax.nn.silu(gate_value) * up_value).astype(jnp.bfloat16)
        return jnp.dot(hidden, shared_down[modal_index], preferred_element_type=jnp.float32)
    is_image = (modality == 1)[:, None]
    shared = jnp.where(is_image, shared_out(0), shared_out(1))
    return (shared + routed).astype(jnp.bfloat16)
```

```python
import functools

import jax
import jax.numpy as jnp
from jax import lax
from jax.experimental import pallas as pl
from jax.experimental.pallas import tpu as pltpu
from jax.sharding import PartitionSpec as P

epsilon = 1e-06
f32 = jnp.float32
bf16 = jnp.bfloat16

EX = 32
TK = 128
MAIN = 16
REST = 4
BLK = 2 * (MAIN + REST)


def normalise(values, gain):
    values = values.astype(f32)
    inv_scale = lax.rsqrt(jnp.mean(values * values, axis=-1, keepdims=True) + epsilon)
    return (values * inv_scale * gain).astype(bf16)


def dot(a, b):
    return jnp.dot(a, b, preferred_element_type=f32)


def dot_t(a, b):
    return lax.dot_general(a, b, (((1,), (1,)), ((), ())), preferred_element_type=f32)


def place_kernel(tok_ref, gain_ref, ids_ref, out_ref, normed_ref, rank_ref):
    normed = normalise(tok_ref[...], gain_ref[...])
    normed_ref[...] = normed
    ids = ids_ref[...]
    expert = lax.broadcasted_iota(jnp.int32, (EX, TK), 0)
    named = ids[0:1] == expert
    for k in range(1, ids.shape[0]):
        named = named | (ids[k : k + 1] == expert)
    ones = jnp.where(named, 1.0, 0.0)
    before = lax.broadcasted_iota(jnp.int32, (TK, TK), 0) < lax.broadcasted_iota(
        jnp.int32, (TK, TK), 1
    )
    rank = dot(ones.astype(bf16), jnp.where(before, 1.0, 0.0).astype(bf16))
    rank = jnp.where(named, rank, -1.0)
    rank_ref[...] = rank
    half = normed.shape[1] // 2
    slot = lax.broadcasted_iota(jnp.int32, (EX, MAIN, TK), 1).astype(f32)
    main = jnp.where(rank[:, None, :] == slot, 1.0, 0.0).astype(bf16).reshape(EX * MAIN, TK)
    row = lax.broadcasted_iota(jnp.int32, (EX, 2 * REST, TK), 1)
    wanted = (row % REST + MAIN).astype(f32)
    rest = jnp.where(rank[:, None, :] == wanted, 1.0, 0.0)
    rest_lo = jnp.where(row < REST, rest, 0.0).astype(bf16).reshape(EX * 2 * REST, TK)
    rest_hi = jnp.where(row >= REST, rest, 0.0).astype(bf16).reshape(EX * 2 * REST, TK)
    step = 256
    for c in range(0, half, step):
        lo = normed[:, c : c + step]
        hi = normed[:, half + c : half + c + step]
        out_ref[:, 0:MAIN, c : c + step] = dot(main, lo).astype(bf16).reshape(EX, MAIN, step)
        out_ref[:, MAIN : 2 * MAIN, c : c + step] = (
            dot(main, hi).astype(bf16).reshape(EX, MAIN, step)
        )
        both = dot(rest_lo, lo) + dot(rest_hi, hi)
        out_ref[:, 2 * MAIN : BLK, c : c + step] = both.reshape(EX, 2 * REST, step).astype(bf16)


def weigh_kernel(normed_ref, router_ref, rank_ref, main_ref, rest_ref):
    rank = rank_ref[...]
    logits = dot_t(router_ref[...], normed_ref[...])
    scores = jnp.where(rank >= 0.0, jax.nn.sigmoid(logits), 0.0)
    weights = scores / jnp.sum(scores, axis=0, keepdims=True)
    slot = lax.broadcasted_iota(jnp.int32, (EX, MAIN, TK), 1).astype(f32)
    main = jnp.where(rank[:, None, :] == slot, weights[:, None, :], 0.0)
    main = main.reshape(EX * MAIN, TK).T
    coarse = main.astype(bf16)
    main_ref[0:TK, :] = coarse
    main_ref[TK:, :] = (main - coarse.astype(f32)).astype(bf16)
    row = lax.broadcasted_iota(jnp.int32, (EX, 2 * REST, TK), 1)
    wanted = (row % REST + MAIN).astype(f32)
    rest = jnp.where(rank[:, None, :] == wanted, weights[:, None, :], 0.0)
    for h in range(2):
        part = jnp.where((row < REST) == (h == 0), rest, 0.0)
        part = part.reshape(EX * 2 * REST, TK).T
        coarse = part.astype(bf16)
        rest_ref[h, 0:TK, :] = coarse
        rest_ref[h, TK:, :] = (part - coarse.astype(f32)).astype(bf16)


def shared_kernel(
    side_ref, normed_ref, other_ref, gain_ref, flag_ref, other_flag_ref, gate_ref, up_ref, down_ref,
    own_ref, pair_ref, near_ref, far_ref, hidden_ref,
):
    other = normalise(other_ref[...], gain_ref[...])
    kinds = gate_ref.shape[0]
    half = own_ref.shape[1]
    for r, rows, flags in ((0, normed_ref[...], flag_ref), (1, other, other_flag_ref)):
        flag = jnp.broadcast_to(flags[...].astype(f32), (TK, TK)).T[:, 0:1]
        for m in range(kinds):
            keep = flag if m == 0 else 1.0 - flag
            gate = dot_t(rows, gate_ref[m])
            up = dot_t(rows, up_ref[m])
            hidden_ref[r, m] = (jax.nn.silu(gate) * up * keep).astype(bf16)
    side = side_ref[0]
    for r in range(2):
        for s in range(2):
            at = (side if s == 0 else 1 - side) * half
            cols = pl.ds(pl.multiple_of(at, half), half)
            part = dot(hidden_ref[r, 0], down_ref[0, :, cols])
            part = part + dot(hidden_ref[r, 1], down_ref[1, :, cols])
            if r == 0 and s == 0:
                own_ref[...] = part
            else:
                target = ((None, pair_ref), (near_ref, far_ref))[r][s]
                target[...] = part.astype(bf16)


def swap4(x):
    return pltpu.roll(x, 4, 1)


def expert_kernel(
    got_ref, gate_hbm, up_hbm, down_hbm, out_hbm,
    gate_ref, up_ref, down_ref, rows_ref, hidden_ref, out_ref, in_sem, out_sem,
):
    width = 2 * got_ref.shape[2]
    half = width // 2
    hid = gate_ref.shape[0]
    cuts = [(c, min(256, hid - c)) for c in range(0, hid, 256)]
    copies = []
    for i, (c, n) in enumerate(cuts):
        copies.append(pltpu.make_async_copy(gate_hbm.at[pl.ds(c, n)], gate_ref.at[pl.ds(c, n)], in_sem.at[2 * i]))
        copies.append(pltpu.make_async_copy(up_hbm.at[pl.ds(c, n)], up_ref.at[pl.ds(c, n)], in_sem.at[2 * i + 1]))
    last = pltpu.make_async_copy(down_hbm, down_ref, in_sem.at[2 * len(cuts)])
    for copy in copies:
        copy.start()
    last.start()
    full = EX * MAIN
    rows_ref[0:full, 0:half] = got_ref[:, 0:MAIN, :].reshape(full, half)
    rows_ref[0:full, half:width] = got_ref[:, MAIN : 2 * MAIN, :].reshape(full, half)
    step = 256
    low = lax.broadcasted_iota(jnp.int32, (EX // 2, 8, step), 1) < REST
    for c in range(0, half, step):
        rest = got_ref[:, 2 * MAIN : BLK, c : c + step].astype(f32).reshape(EX // 2, 2, 8, step)
        even, odd = rest[:, 0], rest[:, 1]
        lo = jnp.where(low, even, swap4(odd))
        hi = jnp.where(low, swap4(even), odd)
        rows_ref[full:, c : c + step] = lo.reshape(EX * REST, step).astype(bf16)
        rows_ref[full:, half + c : half + c + step] = hi.reshape(EX * REST, step).astype(bf16)
    rows = rows_ref[...]
    for i, (c, n) in enumerate(cuts):
        copies[2 * i].wait()
        gate = dot_t(rows, gate_ref[c : c + n, :])
        copies[2 * i + 1].wait()
        up = dot_t(rows, up_ref[c : c + n, :])
        hidden_ref[:, c : c + n] = (jax.nn.silu(gate) * up).astype(bf16)
    last.wait()
    hidden = hidden_ref[...]
    quarter = half // 2
    low = lax.broadcasted_iota(jnp.int32, (EX // 2, 8, quarter), 1) < REST
    sends = []
    for t in range(2):
        rests = []
        for h in range(2):
            at = t * half + h * quarter
            part = dot(hidden, down_ref[:, at : at + quarter])
            out_ref[t, :, h * MAIN : (h + 1) * MAIN, :] = (
                part[0:full].astype(bf16).reshape(EX, MAIN, quarter)
            )
            rests.append(part[full:].reshape(EX // 2, 8, quarter))
        lo, hi = rests
        even = jnp.where(low, lo, swap4(hi))
        odd = jnp.where(low, swap4(lo), hi)
        joined = jnp.stack([even, odd], axis=1).reshape(EX, 8, quarter)
        out_ref[t, :, 2 * MAIN : BLK, :] = joined.astype(bf16)
        send = pltpu.make_async_copy(out_ref.at[t], out_hbm.at[:, t], out_sem.at[t])
        send.start()
        sends.append(send)
    for send in sends:
        send.wait()


def combine_kernel(back_ref, main_ref, rest_ref, own_ref, pair_ref, near_ref, far_ref, out_ref):
    quarter = back_ref.shape[3]
    base = own_ref[...] + pair_ref[...].astype(f32) + near_ref[...].astype(f32)
    base = base + far_ref[...].astype(f32)
    for h in range(2):
        total = None
        for t in range(2):
            rows = back_ref[:, t, h * MAIN : (h + 1) * MAIN, :].reshape(EX * MAIN, quarter)
            part = dot(main_ref[...], rows)
            rest = back_ref[:, t, 2 * MAIN : BLK, :].reshape(EX * 2 * REST, quarter)
            part = part + dot(rest_ref[h], rest)
            total = part if total is None else total + part
        routed = total[0:TK] + total[TK:]
        cols = slice(h * quarter, (h + 1) * quarter)
        out_ref[:, cols] = (base[:, cols] + routed).astype(bf16)


def call(body, out_shape, **kw):
    mib = kw.pop("mib", 32)
    return pl.pallas_call(
        body, out_shape=out_shape, compiler_params=pltpu.CompilerParams(vmem_limit_bytes=mib << 20), **kw
    )


vmem = pl.BlockSpec(memory_space=pltpu.VMEM)
smem = pl.BlockSpec(memory_space=pltpu.SMEM)
hbm = pl.BlockSpec(memory_space=pl.ANY)


def per_device(
    tokens, norm_gain, router, expert_ids, modality,
    expert_gate, expert_up, expert_down, shared_gate, shared_up, shared_down,
):
    sds = jax.ShapeDtypeStruct
    width = tokens.shape[1]
    half = width // 2
    side = lax.axis_index("tensor").astype(jnp.int32).reshape(1)
    gain = norm_gain.reshape(1, width)
    flags = modality.reshape(1, TK)
    swap = [(0, 1), (1, 0)]
    other_tokens = lax.ppermute(tokens, "dp", swap)
    other_flags = lax.ppermute(flags, "dp", swap)

    outgoing, normed, rank = call(
        place_kernel,
        (sds((EX, BLK, half), bf16), sds((TK, width), bf16), sds((EX, TK), f32)),
        name="place",
    )(tokens, gain, expert_ids.T)
    got = lax.all_to_all(outgoing, "expert", 0, 0, tiled=True)

    main, rest = call(
        weigh_kernel,
        (sds((2 * TK, EX * MAIN), bf16), sds((2, 2 * TK, EX * 2 * REST), bf16)),
        name="weigh",
    )(normed, router.T, rank)
    piece = sds((TK, half), bf16)
    own, pair, near, far = call(
        shared_kernel,
        (sds((TK, half), f32), piece, piece, piece),
        in_specs=[smem] + [vmem] * 8,
        scratch_shapes=[pltpu.VMEM((2, 2, TK, shared_gate.shape[2]), bf16)],
        name="shared",
    )(
        side, normed, other_tokens, gain, flags, other_flags,
        shared_gate.swapaxes(1, 2), shared_up.swapaxes(1, 2), shared_down,
    )
    four = ("dp", "tensor")
    pair = lax.ppermute(pair, four, [(i, i ^ 1) for i in range(4)])
    near = lax.ppermute(near, four, [(i, i ^ 2) for i in range(4)])
    far = lax.ppermute(far, four, [(i, i ^ 3) for i in range(4)])

    got, main, rest, own, pair, near, far = lax.optimization_barrier(
        (got, main, rest, own, pair, near, far)
    )

    hid = expert_gate.shape[2]
    rows = EX * (MAIN + REST)
    results = call(
        expert_kernel,
        sds((EX, 2, BLK, half // 2), bf16),
        in_specs=[vmem, hbm, hbm, hbm],
        out_specs=hbm,
        scratch_shapes=[
            pltpu.VMEM((hid, width), bf16),
            pltpu.VMEM((hid, width), bf16),
            pltpu.VMEM((hid, width), bf16),
            pltpu.VMEM((rows, width), bf16),
            pltpu.VMEM((rows, hid), bf16),
            pltpu.VMEM((2, EX, BLK, half // 2), bf16),
            pltpu.SemaphoreType.DMA((7,)),
            pltpu.SemaphoreType.DMA((2,)),
        ],
        mib=56,
        name="expert",
    )(got, expert_gate[0].T, expert_up[0].T, expert_down[0])
    back = lax.all_to_all(
        results.reshape(2 * EX, BLK, half // 2), ("expert", "tensor"), 0, 0, tiled=True
    ).reshape(EX, 2, BLK, half // 2)
    return call(combine_kernel, sds((TK, half), bf16), name="combine")(
        back, main, rest, own, pair, near, far
    )


def solution(mesh):
    in_specs = (
        P(("dp", "expert"), None),
        P(),
        P(),
        P(("dp", "expert"), None),
        P(("dp", "expert")),
        P("expert", None, "tensor"),
        P("expert", None, "tensor"),
        P("expert", "tensor", None),
        P(None, None, ("dp", "tensor")),
        P(None, None, ("dp", "tensor")),
        P(None, ("dp", "tensor"), None),
    )
    out_specs = P(("dp", "expert"), "tensor")
    return jax.shard_map(
        per_device, mesh=mesh, in_specs=in_specs, out_specs=out_specs, check_vma=False
    )
```

```python
import functools

import jax
import jax.numpy as jnp
from jax import lax
from jax.experimental import pallas as pl
from jax.experimental.pallas import tpu as pltpu
from jax.sharding import PartitionSpec as P

epsilon = 1e-06
f32 = jnp.float32
bf16 = jnp.bfloat16

EX = 32
TK = 128
MAIN = 16
REST = 4
BLK = 2 * (MAIN + REST)


CUTS = (0, 256, 1 << 20)


def normalise(values, gain):
    values = values.astype(f32)
    inv_scale = lax.rsqrt(jnp.mean(values * values, axis=-1, keepdims=True) + epsilon)
    return (values * inv_scale * gain).astype(bf16)


def dot(a, b):
    return jnp.dot(a, b, preferred_element_type=f32)


def dot_t(a, b):
    return lax.dot_general(a, b, (((1,), (1,)), ((), ())), preferred_element_type=f32)


def place_kernel(
    tok_hbm, gain_hbm, ids_hbm, out_hbm, normed_ref, rank_ref,
    tok_ref, gain_ref, ids_ref, out_ref, sem, out_sem,
):
    pairs = ((ids_hbm, ids_ref), (tok_hbm, tok_ref), (gain_hbm, gain_ref))
    copies = [pltpu.make_async_copy(a, b, sem.at[i]) for i, (a, b) in enumerate(pairs)]
    for copy in copies:
        copy.start()
    for copy in copies:
        copy.wait()
    normed = normalise(tok_ref[...], gain_ref[...])
    normed_ref[...] = normed
    ids = ids_ref[...]
    expert = lax.broadcasted_iota(jnp.int32, (EX, TK), 0)
    named = ids[0:1] == expert
    for k in range(1, ids.shape[0]):
        named = named | (ids[k : k + 1] == expert)
    ones = jnp.where(named, 1.0, 0.0)
    before = lax.broadcasted_iota(jnp.int32, (TK, TK), 0) < lax.broadcasted_iota(
        jnp.int32, (TK, TK), 1
    )
    rank = dot(ones.astype(bf16), jnp.where(before, 1.0, 0.0).astype(bf16))
    rank = jnp.where(named, rank, -1.0)
    rank_ref[...] = rank
    half = normed.shape[1] // 2
    slot = lax.broadcasted_iota(jnp.int32, (EX, MAIN, TK), 1).astype(f32)
    main = jnp.where(rank[:, None, :] == slot, 1.0, 0.0).astype(bf16).reshape(EX * MAIN, TK)
    row = lax.broadcasted_iota(jnp.int32, (EX, 2 * REST, TK), 1)
    wanted = (row % REST + MAIN).astype(f32)
    rest = jnp.where(rank[:, None, :] == wanted, 1.0, 0.0)
    rest_lo = jnp.where(row < REST, rest, 0.0).astype(bf16).reshape(EX * 2 * REST, TK)
    rest_hi = jnp.where(row >= REST, rest, 0.0).astype(bf16).reshape(EX * 2 * REST, TK)
    step = 256
    sends = []
    for c in range(0, half, step):
        lo = normed[:, c : c + step]
        hi = normed[:, half + c : half + c + step]
        out_ref[:, 0:MAIN, c : c + step] = dot(main, lo).astype(bf16).reshape(EX, MAIN, step)
        out_ref[:, MAIN : 2 * MAIN, c : c + step] = (
            dot(main, hi).astype(bf16).reshape(EX, MAIN, step)
        )
        both = dot(rest_lo, lo) + dot(rest_hi, hi)
        out_ref[:, 2 * MAIN : BLK, c : c + step] = both.reshape(EX, 2 * REST, step).astype(bf16)
        cols = pl.ds(c, step)
        send = pltpu.make_async_copy(
            out_ref.at[:, :, cols], out_hbm.at[:, :, cols], out_sem.at[len(sends)]
        )
        send.start()
        sends.append(send)
    for send in sends:
        send.wait()


def weigh_kernel(normed_ref, router_ref, rank_ref, main_ref, rest_ref):
    rank = rank_ref[...]
    logits = dot_t(router_ref[...], normed_ref[...])
    scores = jnp.where(rank >= 0.0, jax.nn.sigmoid(logits), 0.0)
    weights = scores / jnp.sum(scores, axis=0, keepdims=True)
    slot = lax.broadcasted_iota(jnp.int32, (EX, MAIN, TK), 1).astype(f32)
    main = jnp.where(rank[:, None, :] == slot, weights[:, None, :], 0.0)
    main = main.reshape(EX * MAIN, TK).T
    coarse = main.astype(bf16)
    main_ref[0:TK, :] = coarse
    main_ref[TK:, :] = (main - coarse.astype(f32)).astype(bf16)
    row = lax.broadcasted_iota(jnp.int32, (EX, 2 * REST, TK), 1)
    wanted = (row % REST + MAIN).astype(f32)
    rest = jnp.where(rank[:, None, :] == wanted, weights[:, None, :], 0.0)
    for h in range(2):
        part = jnp.where((row < REST) == (h == 0), rest, 0.0)
        part = part.reshape(EX * 2 * REST, TK).T
        coarse = part.astype(bf16)
        rest_ref[h, 0:TK, :] = coarse
        rest_ref[h, TK:, :] = (part - coarse.astype(f32)).astype(bf16)


def shared_kernel(
    side_ref, normed_ref, other_ref, gain_ref, flag_ref, other_flag_ref, gate_ref, up_ref, down_ref,
    own_ref, pair_ref, near_ref, far_ref, hidden_ref,
):
    other = normalise(other_ref[...], gain_ref[...])
    kinds = gate_ref.shape[0]
    half = own_ref.shape[1]
    for r, rows, flags in ((0, normed_ref[...], flag_ref), (1, other, other_flag_ref)):
        flag = jnp.broadcast_to(flags[...].astype(f32), (TK, TK)).T[:, 0:1]
        for m in range(kinds):
            keep = flag if m == 0 else 1.0 - flag
            gate = dot_t(rows, gate_ref[m])
            up = dot_t(rows, up_ref[m])
            hidden_ref[r, m] = (jax.nn.silu(gate) * up * keep).astype(bf16)
    side = side_ref[0]
    for r in range(2):
        for s in range(2):
            at = (side if s == 0 else 1 - side) * half
            cols = pl.ds(pl.multiple_of(at, half), half)
            part = dot(hidden_ref[r, 0], down_ref[0, :, cols])
            part = part + dot(hidden_ref[r, 1], down_ref[1, :, cols])
            if r == 0 and s == 0:
                own_ref[...] = part
            else:
                target = ((None, pair_ref), (near_ref, far_ref))[r][s]
                target[...] = part.astype(bf16)


def swap4(x):
    return pltpu.roll(x, 4, 1)


def expert_kernel(
    got_ref, gate_hbm, up_hbm, down_hbm, out_hbm,
    gate_ref, up_ref, down_ref, rows_ref, hidden_ref, out_ref, in_sem, sem,
):
    width = 2 * got_ref.shape[2]
    half = width // 2
    hid = gate_ref.shape[0]
    full = EX * MAIN
    quarter = half // 2
    cuts = [(c, min(CUTS[i + 1], hid) - c) for i, c in enumerate(CUTS[:-1])]
    loads = []
    for c, n in cuts:
        cut = pl.ds(c, n)
        loads.append([(gate_hbm.at[cut], gate_ref.at[cut]), (up_hbm.at[cut], up_ref.at[cut])])
    loads.append([(down_hbm, down_ref)])
    count = 0
    for i, group in enumerate(loads):
        for j, (source, target) in enumerate(group):
            group[j] = pltpu.make_async_copy(source, target, in_sem.at[count])
            count += 1

    for group in loads:
        for copy in group:
            copy.start()
    rows_ref[0:full, 0:half] = got_ref[:, 0:MAIN, :].reshape(full, half)
    rows_ref[0:full, half:width] = got_ref[:, MAIN : 2 * MAIN, :].reshape(full, half)
    step = 256
    low = lax.broadcasted_iota(jnp.int32, (EX // 2, 8, step), 1) < REST
    for c in range(0, half, step):
        rest = got_ref[:, 2 * MAIN : BLK, c : c + step].astype(f32).reshape(EX // 2, 2, 8, step)
        even, odd = rest[:, 0], rest[:, 1]
        lo = jnp.where(low, even, swap4(odd))
        hi = jnp.where(low, swap4(even), odd)
        rows_ref[full:, c : c + step] = lo.reshape(EX * REST, step).astype(bf16)
        rows_ref[full:, half + c : half + c + step] = hi.reshape(EX * REST, step).astype(bf16)
    for (c, n), group in zip(cuts, loads):
        for copy in group:
            copy.wait()
        gate = dot_t(rows_ref[...], gate_ref[c : c + n, :])
        up = dot_t(rows_ref[...], up_ref[c : c + n, :])
        hidden_ref[:, c : c + n] = (jax.nn.silu(gate) * up).astype(bf16)
    loads[-1][0].wait()
    low = lax.broadcasted_iota(jnp.int32, (EX // 2, 8, quarter), 1) < REST
    sends = []

    def send(t, first, count):
        rows = pl.ds(first, count)
        copy = pltpu.make_async_copy(
            out_ref.at[:, t, rows, :], out_hbm.at[:, t, rows, :], sem.at[len(sends)]
        )
        copy.start()
        sends.append(copy)

    for t in range(2):
        rests = []
        for h in range(2):
            at = t * half + h * quarter
            part = dot(hidden_ref[...], down_ref[:, at : at + quarter])
            out_ref[:, t, h * MAIN : (h + 1) * MAIN, :] = (
                part[0:full].astype(bf16).reshape(EX, MAIN, quarter)
            )
            if h == 0:
                send(t, 0, MAIN)
            rests.append(part[full:].reshape(EX // 2, 8, quarter))
        lo, hi = rests
        even = jnp.where(low, lo, swap4(hi))
        odd = jnp.where(low, swap4(lo), hi)
        joined = jnp.stack([even, odd], axis=1).reshape(EX, 8, quarter)
        out_ref[:, t, 2 * MAIN : BLK, :] = joined.astype(bf16)
        send(t, MAIN, BLK - MAIN)
    for copy in sends:
        copy.wait()


def combine_kernel(
    back_ref, main_hbm, rest_hbm, own_hbm, pair_hbm, near_hbm, far_hbm, out_ref,
    main_ref, rest_ref, own_ref, pair_ref, near_ref, far_ref, sem,
):
    sources = (main_hbm, rest_hbm, own_hbm, pair_hbm, near_hbm, far_hbm)
    targets = (main_ref, rest_ref, own_ref, pair_ref, near_ref, far_ref)
    copies = []
    for i, (source, target) in enumerate(zip(sources, targets)):
        copies.append(pltpu.make_async_copy(source, target, sem.at[i]))
        copies[i].start()
    quarter = back_ref.shape[3]
    copies[0].wait()
    copies[1].wait()
    routed = []
    for h in range(2):
        total = None
        for t in range(2):
            rows = back_ref[:, t, h * MAIN : (h + 1) * MAIN, :].reshape(EX * MAIN, quarter)
            part = dot(main_ref[...], rows)
            rest = back_ref[:, t, 2 * MAIN : BLK, :].reshape(EX * 2 * REST, quarter)
            part = part + dot(rest_ref[h], rest)
            total = part if total is None else total + part
        routed.append(total[0:TK] + total[TK:])
    for copy in copies[2:]:
        copy.wait()
    base = own_ref[...] + pair_ref[...].astype(f32) + near_ref[...].astype(f32)
    base = base + far_ref[...].astype(f32)
    for h in range(2):
        cols = slice(h * quarter, (h + 1) * quarter)
        out_ref[:, cols] = (base[:, cols] + routed[h]).astype(bf16)


def call(body, out_shape, **kw):
    mib = kw.pop("mib", 16)
    return pl.pallas_call(
        body, out_shape=out_shape, compiler_params=pltpu.CompilerParams(vmem_limit_bytes=mib << 20), **kw
    )


vmem = pl.BlockSpec(memory_space=pltpu.VMEM)
smem = pl.BlockSpec(memory_space=pltpu.SMEM)
hbm = pl.BlockSpec(memory_space=pl.ANY)


def in_hbm(x):
    return pltpu.with_memory_space_constraint(x, pltpu.HBM)


def per_device(
    tokens, norm_gain, router, expert_ids, modality,
    expert_gate, expert_up, expert_down, shared_gate, shared_up, shared_down,
):
    sds = jax.ShapeDtypeStruct
    width = tokens.shape[1]
    half = width // 2
    side = lax.axis_index("tensor").astype(jnp.int32).reshape(1)
    gain = norm_gain.reshape(1, width)
    flags = modality.reshape(1, TK)
    swap = [(0, 1), (1, 0)]
    other_tokens = lax.ppermute(tokens, "dp", swap)
    other_flags = lax.ppermute(flags, "dp", swap)

    outgoing, normed, rank = call(
        place_kernel,
        (pltpu.HBM((EX, BLK, half), bf16), sds((TK, width), bf16), sds((EX, TK), f32)),
        in_specs=[hbm] * 3,
        out_specs=[hbm, vmem, vmem],
        scratch_shapes=[
            pltpu.VMEM((TK, width), bf16),
            pltpu.VMEM((1, width), f32),
            pltpu.VMEM((expert_ids.shape[1], TK), jnp.int32),
            pltpu.VMEM((EX, BLK, half), bf16),
            pltpu.SemaphoreType.DMA((3,)),
            pltpu.SemaphoreType.DMA((4,)),
        ],
        name="place",
    )(in_hbm(tokens), in_hbm(gain), in_hbm(expert_ids.T))
    got = lax.all_to_all(outgoing, "expert", 0, 0, tiled=True)

    hid = expert_gate.shape[2]
    main, rest = call(
        weigh_kernel,
        (
            pltpu.HBM((2 * TK, EX * MAIN), bf16),
            pltpu.HBM((2, 2 * TK, EX * 2 * REST), bf16),
        ),
        name="weigh",
    )(normed, router.T, rank)
    piece = pltpu.HBM((TK, half), bf16)
    own, pair, near, far = call(
        shared_kernel,
        (pltpu.HBM((TK, half), f32), piece, piece, piece),
        in_specs=[smem] + [vmem] * 8,
        scratch_shapes=[pltpu.VMEM((2, 2, TK, shared_gate.shape[2]), bf16)],
        name="shared",
    )(
        side, normed, other_tokens, gain, flags, other_flags,
        shared_gate.swapaxes(1, 2), shared_up.swapaxes(1, 2), shared_down,
    )
    got, main, rest, own, pair, near, far = lax.optimization_barrier(
        (got, main, rest, own, pair, near, far)
    )
    four = ("dp", "tensor")
    pair = lax.ppermute(pair, four, [(i, i ^ 1) for i in range(4)])
    near = lax.ppermute(near, four, [(i, i ^ 2) for i in range(4)])
    far = lax.ppermute(far, four, [(i, i ^ 3) for i in range(4)])

    hid = expert_gate.shape[2]
    rows = EX * (MAIN + REST)
    results = call(
        expert_kernel,
        pltpu.HBM((EX, 2, BLK, half // 2), bf16),
        in_specs=[vmem, hbm, hbm, hbm],
        out_specs=hbm,
        scratch_shapes=[
            pltpu.VMEM((hid, width), bf16),
            pltpu.VMEM((hid, width), bf16),
            pltpu.VMEM((hid, width), bf16),
            pltpu.VMEM((rows, width), bf16),
            pltpu.VMEM((rows, hid), bf16),
            pltpu.VMEM((EX, 2, BLK, half // 2), bf16),
            pltpu.SemaphoreType.DMA((2 * len(CUTS) - 1,)),
            pltpu.SemaphoreType.DMA((4,)),
        ],
        mib=32,
        name="expert",
    )(got, in_hbm(expert_gate[0].T), in_hbm(expert_up[0].T), in_hbm(expert_down[0]))
    back = lax.all_to_all(
        results.reshape(2 * EX, BLK, half // 2), ("expert", "tensor"), 0, 0, tiled=True
    ).reshape(EX, 2, BLK, half // 2)
    fixed = (main, rest, own, pair, near, far)
    return call(
        combine_kernel,
        sds((TK, half), bf16),
        in_specs=[vmem] + [hbm] * 6,
        scratch_shapes=[pltpu.VMEM(x.shape, x.dtype) for x in fixed]
        + [pltpu.SemaphoreType.DMA((6,))],
        name="combine",
    )(back, *[in_hbm(x) for x in fixed])


def solution(mesh):
    in_specs = (
        P(("dp", "expert"), None),
        P(),
        P(),
        P(("dp", "expert"), None),
        P(("dp", "expert")),
        P("expert", None, "tensor"),
        P("expert", None, "tensor"),
        P("expert", "tensor", None),
        P(None, None, ("dp", "tensor")),
        P(None, None, ("dp", "tensor")),
        P(None, ("dp", "tensor"), None),
    )
    out_specs = P(("dp", "expert"), "tensor")
    return jax.shard_map(
        per_device, mesh=mesh, in_specs=in_specs, out_specs=out_specs, check_vma=False
    )
```

```python
import functools

import jax
import jax.numpy as jnp
from jax import lax
from jax.experimental import pallas as pl
from jax.experimental.pallas import tpu as pltpu
from jax.sharding import PartitionSpec as P

epsilon = 1e-06
f32 = jnp.float32
bf16 = jnp.bfloat16

EX = 32
TK = 128
MAIN = 16
REST = 4
BLK = 2 * (MAIN + REST)


CUTS = (0, 256, 1 << 20)


def normalise(values, gain):
    values = values.astype(f32)
    inv_scale = lax.rsqrt(jnp.mean(values * values, axis=-1, keepdims=True) + epsilon)
    return (values * inv_scale * gain).astype(bf16)


def dot(a, b):
    return jnp.dot(a, b, preferred_element_type=f32)


def dot_t(a, b):
    return lax.dot_general(a, b, (((1,), (1,)), ((), ())), preferred_element_type=f32)


def slot_ranks(ids):
    expert = lax.broadcasted_iota(jnp.int32, (EX, TK), 0)
    named = ids[0:1] == expert
    for k in range(1, ids.shape[0]):
        named = named | (ids[k : k + 1] == expert)
    ones = jnp.where(named, 1.0, 0.0)
    before = lax.broadcasted_iota(jnp.int32, (TK, TK), 0) < lax.broadcasted_iota(
        jnp.int32, (TK, TK), 1
    )
    rank = dot(ones.astype(bf16), jnp.where(before, 1.0, 0.0).astype(bf16))
    return jnp.where(named, rank, -1.0)


def place_kernel(
    tok_hbm, gain_hbm, ids_hbm, out_hbm, tok_ref, gain_ref, ids_ref, out_ref, sem, out_sem
):
    pairs = ((ids_hbm, ids_ref), (gain_hbm, gain_ref), (tok_hbm, tok_ref))
    copies = [pltpu.make_async_copy(a, b, sem.at[i]) for i, (a, b) in enumerate(pairs)]
    for copy in copies:
        copy.start()
    for copy in copies:
        copy.wait()
    rank = slot_ranks(ids_ref[...])
    normed = normalise(tok_ref[...], gain_ref[...])
    half = normed.shape[1] // 2
    slot = lax.broadcasted_iota(jnp.int32, (EX, MAIN, TK), 1).astype(f32)
    main = jnp.where(rank[:, None, :] == slot, 1.0, 0.0).astype(bf16).reshape(EX * MAIN, TK)
    row = lax.broadcasted_iota(jnp.int32, (EX, 2 * REST, TK), 1)
    wanted = (row % REST + MAIN).astype(f32)
    rest = jnp.where(rank[:, None, :] == wanted, 1.0, 0.0)
    rest_lo = jnp.where(row < REST, rest, 0.0).astype(bf16).reshape(EX * 2 * REST, TK)
    rest_hi = jnp.where(row >= REST, rest, 0.0).astype(bf16).reshape(EX * 2 * REST, TK)
    step = 256
    sends = []
    for c in range(0, half, step):
        lo = normed[:, c : c + step]
        hi = normed[:, half + c : half + c + step]
        out_ref[:, 0:MAIN, c : c + step] = dot(main, lo).astype(bf16).reshape(EX, MAIN, step)
        out_ref[:, MAIN : 2 * MAIN, c : c + step] = (
            dot(main, hi).astype(bf16).reshape(EX, MAIN, step)
        )
        both = dot(rest_lo, lo) + dot(rest_hi, hi)
        out_ref[:, 2 * MAIN : BLK, c : c + step] = both.reshape(EX, 2 * REST, step).astype(bf16)
        cols = pl.ds(c, step)
        send = pltpu.make_async_copy(
            out_ref.at[:, :, cols], out_hbm.at[:, :, cols], out_sem.at[len(sends)]
        )
        send.start()
        sends.append(send)
    for send in sends:
        send.wait()


def weigh_kernel(
    side_ref, tok_ref, gain_ref, ids_ref, router_ref, flag_ref, gate_hbm, up_hbm, down_hbm,
    main_ref, rest_ref, own_ref, pair_ref, gate_ref, up_ref, down_ref, hidden_ref, sem,
):
    pairs = ((gate_hbm, gate_ref), (up_hbm, up_ref), (down_hbm, down_ref))
    copies = [pltpu.make_async_copy(a, b, sem.at[i]) for i, (a, b) in enumerate(pairs)]
    for copy in copies:
        copy.start()
    rank = slot_ranks(ids_ref[...])
    normed = normalise(tok_ref[...], gain_ref[...])
    logits = dot_t(router_ref[...], normed)
    scores = jnp.where(rank >= 0.0, jax.nn.sigmoid(logits), 0.0)
    weights = scores / jnp.sum(scores, axis=0, keepdims=True)
    slot = lax.broadcasted_iota(jnp.int32, (EX, MAIN, TK), 1).astype(f32)
    main = jnp.where(rank[:, None, :] == slot, weights[:, None, :], 0.0)
    main = main.reshape(EX * MAIN, TK).T
    coarse = main.astype(bf16)
    main_ref[0:TK, :] = coarse
    main_ref[TK:, :] = (main - coarse.astype(f32)).astype(bf16)
    row = lax.broadcasted_iota(jnp.int32, (EX, 2 * REST, TK), 1)
    wanted = (row % REST + MAIN).astype(f32)
    rest = jnp.where(rank[:, None, :] == wanted, weights[:, None, :], 0.0)
    for h in range(2):
        part = jnp.where((row < REST) == (h == 0), rest, 0.0)
        part = part.reshape(EX * 2 * REST, TK).T
        coarse = part.astype(bf16)
        rest_ref[h, 0:TK, :] = coarse
        rest_ref[h, TK:, :] = (part - coarse.astype(f32)).astype(bf16)
    for copy in copies:
        copy.wait()
    shared_terms(
        side_ref, normed, flag_ref, gate_ref, up_ref, down_ref, hidden_ref,
        own_ref, pair_ref,
    )


def shared_terms(
    side_ref, rows, flag_ref, gate_ref, up_ref, down_ref, hidden_ref, same_ref, cross_ref
):
    flag = jnp.broadcast_to(flag_ref[...].astype(f32), (TK, TK)).T[:, 0:1]
    for m in range(gate_ref.shape[0]):
        keep = flag if m == 0 else 1.0 - flag
        gate = dot_t(rows, gate_ref[m])
        up = dot_t(rows, up_ref[m])
        hidden_ref[m] = (jax.nn.silu(gate) * up * keep).astype(bf16)
    side = side_ref[0]
    half = same_ref.shape[1]
    for target, at in ((cross_ref, 1 - side), (same_ref, side)):
        cols = pl.ds(pl.multiple_of(at * half, half), half)
        part = dot(hidden_ref[0], down_ref[0, :, cols])
        part = part + dot(hidden_ref[1], down_ref[1, :, cols])
        target[...] = part.astype(target.dtype)


def shared_kernel(
    side_ref, other_ref, gain_ref, flag_ref, gate_ref, up_ref, down_ref,
    near_ref, far_ref, hidden_ref,
):
    rows = normalise(other_ref[...], gain_ref[...])
    shared_terms(
        side_ref, rows, flag_ref, gate_ref, up_ref, down_ref, hidden_ref, near_ref, far_ref
    )


def swap4(x):
    return pltpu.roll(x, 4, 1)


def expert_kernel(
    got_ref, gate_hbm, up_hbm, down_hbm, out_hbm,
    gate_ref, up_ref, down_ref, rows_ref, hidden_ref, out_ref, in_sem, sem,
):
    width = 2 * got_ref.shape[2]
    half = width // 2
    hid = gate_ref.shape[0]
    full = EX * MAIN
    quarter = half // 2
    cuts = [(c, min(CUTS[i + 1], hid) - c) for i, c in enumerate(CUTS[:-1])]
    loads = []
    for c, n in cuts:
        cut = pl.ds(c, n)
        loads.append([(gate_hbm.at[cut], gate_ref.at[cut]), (up_hbm.at[cut], up_ref.at[cut])])
    loads.append([(down_hbm, down_ref)])
    count = 0
    for i, group in enumerate(loads):
        for j, (source, target) in enumerate(group):
            group[j] = pltpu.make_async_copy(source, target, in_sem.at[count])
            count += 1

    for group in loads:
        for copy in group:
            copy.start()
    rows_ref[0:full, 0:half] = got_ref[:, 0:MAIN, :].reshape(full, half)
    rows_ref[0:full, half:width] = got_ref[:, MAIN : 2 * MAIN, :].reshape(full, half)
    step = 256
    low = lax.broadcasted_iota(jnp.int32, (EX // 2, 8, step), 1) < REST
    for c in range(0, half, step):
        rest = got_ref[:, 2 * MAIN : BLK, c : c + step].astype(f32).reshape(EX // 2, 2, 8, step)
        even, odd = rest[:, 0], rest[:, 1]
        lo = jnp.where(low, even, swap4(odd))
        hi = jnp.where(low, swap4(even), odd)
        rows_ref[full:, c : c + step] = lo.reshape(EX * REST, step).astype(bf16)
        rows_ref[full:, half + c : half + c + step] = hi.reshape(EX * REST, step).astype(bf16)
    for (c, n), group in zip(cuts, loads):
        for copy in group:
            copy.wait()
        gate = dot_t(rows_ref[...], gate_ref[c : c + n, :])
        up = dot_t(rows_ref[...], up_ref[c : c + n, :])
        hidden_ref[:, c : c + n] = (jax.nn.silu(gate) * up).astype(bf16)
    loads[-1][0].wait()
    low = lax.broadcasted_iota(jnp.int32, (EX // 2, 8, quarter), 1) < REST
    sends = []

    def send(t, first, count):
        rows = pl.ds(first, count)
        copy = pltpu.make_async_copy(
            out_ref.at[:, t, rows, :], out_hbm.at[:, t, rows, :], sem.at[len(sends)]
        )
        copy.start()
        sends.append(copy)

    for t in range(2):
        rests = []
        for h in range(2):
            at = t * half + h * quarter
            part = dot(hidden_ref[...], down_ref[:, at : at + quarter])
            out_ref[:, t, h * MAIN : (h + 1) * MAIN, :] = (
                part[0:full].astype(bf16).reshape(EX, MAIN, quarter)
            )
            if h == 0:
                send(t, 0, MAIN)
            rests.append(part[full:].reshape(EX // 2, 8, quarter))
        lo, hi = rests
        even = jnp.where(low, lo, swap4(hi))
        odd = jnp.where(low, swap4(lo), hi)
        joined = jnp.stack([even, odd], axis=1).reshape(EX, 8, quarter)
        out_ref[:, t, 2 * MAIN : BLK, :] = joined.astype(bf16)
        send(t, MAIN, BLK - MAIN)
    for copy in sends:
        copy.wait()


def combine_kernel(back_ref, main_ref, rest_ref, base_hbm, out_ref, base_ref, sem):
    copy = pltpu.make_async_copy(base_hbm, base_ref, sem)
    copy.start()
    quarter = back_ref.shape[3]
    routed = []
    for h in range(2):
        total = None
        for t in range(2):
            rows = back_ref[:, t, h * MAIN : (h + 1) * MAIN, :].reshape(EX * MAIN, quarter)
            part = dot(main_ref[...], rows)
            rest = back_ref[:, t, 2 * MAIN : BLK, :].reshape(EX * 2 * REST, quarter)
            part = part + dot(rest_ref[h], rest)
            total = part if total is None else total + part
        routed.append(total[0:TK] + total[TK:])
    copy.wait()
    for h in range(2):
        cols = slice(h * quarter, (h + 1) * quarter)
        out_ref[:, cols] = (base_ref[:, cols] + routed[h]).astype(bf16)


def call(body, out_shape, **kw):
    mib = kw.pop("mib", 16)
    return pl.pallas_call(
        body, out_shape=out_shape, compiler_params=pltpu.CompilerParams(vmem_limit_bytes=mib << 20), **kw
    )


vmem = pl.BlockSpec(memory_space=pltpu.VMEM)
smem = pl.BlockSpec(memory_space=pltpu.SMEM)
hbm = pl.BlockSpec(memory_space=pl.ANY)


def in_hbm(x):
    return pltpu.with_memory_space_constraint(x, pltpu.HBM)


def in_vmem(x):
    return pltpu.with_memory_space_constraint(x, pltpu.VMEM)


def per_device(
    tokens, norm_gain, router, expert_ids, modality,
    expert_gate, expert_up, expert_down, shared_gate, shared_up, shared_down,
):
    sds = jax.ShapeDtypeStruct
    width = tokens.shape[1]
    half = width // 2
    side = lax.axis_index("tensor").astype(jnp.int32).reshape(1)
    gain = norm_gain.reshape(1, width)
    flags = modality.reshape(1, TK)
    swap = [(0, 1), (1, 0)]
    other_tokens = lax.ppermute(tokens, "dp", swap)
    other_flags = lax.ppermute(flags, "dp", swap)

    outgoing = call(
        place_kernel,
        pltpu.HBM((EX, BLK, half), bf16),
        in_specs=[hbm] * 3,
        out_specs=hbm,
        scratch_shapes=[
            pltpu.VMEM((TK, width), bf16),
            pltpu.VMEM((1, width), f32),
            pltpu.VMEM((expert_ids.shape[1], TK), jnp.int32),
            pltpu.VMEM((EX, BLK, half), bf16),
            pltpu.SemaphoreType.DMA((3,)),
            pltpu.SemaphoreType.DMA((4,)),
        ],
        name="place",
    )(in_hbm(tokens), in_hbm(gain), in_hbm(expert_ids.T))
    got = lax.all_to_all(outgoing, "expert", 0, 0, tiled=True)

    hid = expert_gate.shape[2]
    piece = pltpu.HBM((TK, half), bf16)
    hidden = pltpu.VMEM((2, TK, shared_gate.shape[2]), bf16)
    part = pltpu.VMEM(shared_down.shape, bf16)
    main, rest, own, pair, *weights = call(
        weigh_kernel,
        (
            sds((2 * TK, EX * MAIN), bf16),
            sds((2, 2 * TK, EX * 2 * REST), bf16),
            pltpu.HBM((TK, half), f32),
            piece,
            part,
            part,
            part,
        ),
        in_specs=[smem] + [vmem] * 5 + [hbm] * 3,
        scratch_shapes=[hidden, pltpu.SemaphoreType.DMA((3,))],
        name="weigh",
    )(
        side, tokens, gain, expert_ids.T, router.T, flags,
        in_hbm(shared_gate.swapaxes(1, 2)), in_hbm(shared_up.swapaxes(1, 2)), in_hbm(shared_down),
    )
    four = ("dp", "tensor")
    pair = lax.ppermute(pair, four, [(i, i ^ 1) for i in range(4)])
    near, far = call(
        shared_kernel,
        (piece, piece),
        in_specs=[smem] + [vmem] * 6,
        scratch_shapes=[hidden],
        name="shared",
    )(side, other_tokens, gain, other_flags, *[in_vmem(x) for x in weights])
    near = lax.ppermute(near, four, [(i, i ^ 2) for i in range(4)])
    far = lax.ppermute(far, four, [(i, i ^ 3) for i in range(4)])
    got, main, rest, own, pair, near, far = lax.optimization_barrier(
        (got, main, rest, own, pair, near, far)
    )
    base = own + pair.astype(f32) + near.astype(f32) + far.astype(f32)

    hid = expert_gate.shape[2]
    rows = EX * (MAIN + REST)
    results = call(
        expert_kernel,
        pltpu.HBM((EX, 2, BLK, half // 2), bf16),
        in_specs=[vmem, hbm, hbm, hbm],
        out_specs=hbm,
        scratch_shapes=[
            pltpu.VMEM((hid, width), bf16),
            pltpu.VMEM((hid, width), bf16),
            pltpu.VMEM((hid, width), bf16),
            pltpu.VMEM((rows, width), bf16),
            pltpu.VMEM((rows, hid), bf16),
            pltpu.VMEM((EX, 2, BLK, half // 2), bf16),
            pltpu.SemaphoreType.DMA((2 * len(CUTS) - 1,)),
            pltpu.SemaphoreType.DMA((4,)),
        ],
        mib=32,
        name="expert",
    )(got, in_hbm(expert_gate[0].T), in_hbm(expert_up[0].T), in_hbm(expert_down[0]))
    back = lax.all_to_all(
        results.reshape(2 * EX, BLK, half // 2), ("expert", "tensor"), 0, 0, tiled=True
    ).reshape(EX, 2, BLK, half // 2)
    return call(
        combine_kernel,
        sds((TK, half), bf16),
        in_specs=[vmem] * 3 + [hbm],
        scratch_shapes=[pltpu.VMEM((TK, half), f32), pltpu.SemaphoreType.DMA],
        name="combine",
    )(back, main, rest, in_hbm(base))


def solution(mesh):
    in_specs = (
        P(("dp", "expert"), None),
        P(),
        P(),
        P(("dp", "expert"), None),
        P(("dp", "expert")),
        P("expert", None, "tensor"),
        P("expert", None, "tensor"),
        P("expert", "tensor", None),
        P(None, None, ("dp", "tensor")),
        P(None, None, ("dp", "tensor")),
        P(None, ("dp", "tensor"), None),
    )
    out_specs = P(("dp", "expert"), "tensor")
    return jax.shard_map(
        per_device, mesh=mesh, in_specs=in_specs, out_specs=out_specs, check_vma=False
    )
```

```python
import functools

import jax
import jax.numpy as jnp
from jax import lax
from jax.experimental import pallas as pl
from jax.experimental.pallas import tpu as pltpu
from jax.sharding import PartitionSpec as P

epsilon = 1e-06
f32 = jnp.float32
bf16 = jnp.bfloat16

EX = 32
TK = 128
MAIN = 16
REST = 4
BLK = 2 * (MAIN + REST)


CUTS = (0, 256, 1 << 20)


def normalise(values, gain):
    values = values.astype(f32)
    inv_scale = lax.rsqrt(jnp.mean(values * values, axis=-1, keepdims=True) + epsilon)
    return (values * inv_scale * gain).astype(bf16)


def dot(a, b):
    return jnp.dot(a, b, preferred_element_type=f32)


def dot_t(a, b):
    return lax.dot_general(a, b, (((1,), (1,)), ((), ())), preferred_element_type=f32)


def slot_ranks(ids):
    expert = lax.broadcasted_iota(jnp.int32, (EX, TK), 0)
    named = ids[0:1] == expert
    for k in range(1, ids.shape[0]):
        named = named | (ids[k : k + 1] == expert)
    ones = jnp.where(named, 1.0, 0.0)
    before = lax.broadcasted_iota(jnp.int32, (TK, TK), 0) < lax.broadcasted_iota(
        jnp.int32, (TK, TK), 1
    )
    rank = dot(ones.astype(bf16), jnp.where(before, 1.0, 0.0).astype(bf16))
    return jnp.where(named, rank, -1.0)


def place_kernel(
    tok_hbm, gain_hbm, ids_hbm, out_hbm, tok_ref, gain_ref, ids_ref, out_ref, sem, out_sem
):
    pairs = ((ids_hbm, ids_ref), (gain_hbm, gain_ref), (tok_hbm, tok_ref))
    copies = [pltpu.make_async_copy(a, b, sem.at[i]) for i, (a, b) in enumerate(pairs)]
    for copy in copies:
        copy.start()
    copies[0].wait()
    rank = slot_ranks(ids_ref[...])
    half = tok_ref.shape[1] // 2
    slot = lax.broadcasted_iota(jnp.int32, (EX, MAIN, TK), 1).astype(f32)
    main = jnp.where(rank[:, None, :] == slot, 1.0, 0.0).astype(bf16).reshape(EX * MAIN, TK)
    row = lax.broadcasted_iota(jnp.int32, (EX, 2 * REST, TK), 1)
    wanted = (row % REST + MAIN).astype(f32)
    rest = jnp.where(rank[:, None, :] == wanted, 1.0, 0.0)
    rest_lo = jnp.where(row < REST, rest, 0.0).astype(bf16).reshape(EX * 2 * REST, TK)
    rest_hi = jnp.where(row >= REST, rest, 0.0).astype(bf16).reshape(EX * 2 * REST, TK)
    rest = jnp.concatenate([rest_lo, rest_hi], axis=1)
    for copy in copies[1:]:
        copy.wait()
    normed = normalise(tok_ref[...], gain_ref[...])
    step = 256
    sends = []
    for c in range(0, half, step):
        lo = normed[:, c : c + step]
        hi = normed[:, half + c : half + c + step]
        out_ref[:, 0:MAIN, c : c + step] = dot(main, lo).astype(bf16).reshape(EX, MAIN, step)
        out_ref[:, MAIN : 2 * MAIN, c : c + step] = (
            dot(main, hi).astype(bf16).reshape(EX, MAIN, step)
        )
        both = dot(rest, jnp.concatenate([lo, hi], axis=0))
        out_ref[:, 2 * MAIN : BLK, c : c + step] = both.reshape(EX, 2 * REST, step).astype(bf16)
        cols = pl.ds(c, step)
        send = pltpu.make_async_copy(
            out_ref.at[:, :, cols], out_hbm.at[:, :, cols], out_sem.at[len(sends)]
        )
        send.start()
        sends.append(send)
    for send in sends:
        send.wait()


def weigh_kernel(
    side_ref, tok_ref, gain_ref, ids_ref, router_ref, flag_ref, gate_hbm, up_hbm, down_hbm,
    main_ref, rest_ref, own_ref, pair_ref, gate_ref, up_ref, down_ref, hidden_ref, sem,
):
    pairs = ((gate_hbm, gate_ref), (up_hbm, up_ref), (down_hbm, down_ref))
    copies = [pltpu.make_async_copy(a, b, sem.at[i]) for i, (a, b) in enumerate(pairs)]
    for copy in copies:
        copy.start()
    rank = slot_ranks(ids_ref[...])
    normed = normalise(tok_ref[...], gain_ref[...])
    logits = dot_t(router_ref[...], normed)
    scores = jnp.where(rank >= 0.0, jax.nn.sigmoid(logits), 0.0)
    weights = scores / jnp.sum(scores, axis=0, keepdims=True)
    slot = lax.broadcasted_iota(jnp.int32, (EX, MAIN, TK), 1).astype(f32)
    main = jnp.where(rank[:, None, :] == slot, weights[:, None, :], 0.0)
    main = main.reshape(EX * MAIN, TK).T
    coarse = main.astype(bf16)
    main_ref[0:TK, :] = coarse
    main_ref[TK:, :] = (main - coarse.astype(f32)).astype(bf16)
    row = lax.broadcasted_iota(jnp.int32, (EX, 2 * REST, TK), 1)
    wanted = (row % REST + MAIN).astype(f32)
    rest = jnp.where(rank[:, None, :] == wanted, weights[:, None, :], 0.0)
    rest = rest.reshape(EX * 2 * REST, TK).T
    coarse = rest.astype(bf16)
    rest_ref[0:TK, :] = coarse
    rest_ref[TK:, :] = (rest - coarse.astype(f32)).astype(bf16)
    for copy in copies:
        copy.wait()
    shared_terms(
        side_ref, normed, flag_ref, gate_ref, up_ref, down_ref, hidden_ref,
        own_ref, pair_ref,
    )


def shared_terms(
    side_ref, rows, flag_ref, gate_ref, up_ref, down_ref, hidden_ref, same_ref, cross_ref
):
    flag = jnp.broadcast_to(flag_ref[...].astype(f32), (TK, TK)).T[:, 0:1]
    for m in range(gate_ref.shape[0]):
        keep = flag if m == 0 else 1.0 - flag
        gate = dot_t(rows, gate_ref[m])
        up = dot_t(rows, up_ref[m])
        hidden_ref[m] = (jax.nn.silu(gate) * up * keep).astype(bf16)
    side = side_ref[0]
    half = same_ref.shape[1]
    for target, at in ((cross_ref, 1 - side), (same_ref, side)):
        cols = pl.ds(pl.multiple_of(at * half, half), half)
        part = dot(hidden_ref[0], down_ref[0, :, cols])
        part = part + dot(hidden_ref[1], down_ref[1, :, cols])
        target[...] = part.astype(target.dtype)


def shared_kernel(
    side_ref, other_ref, gain_ref, flag_ref, gate_ref, up_ref, down_ref,
    near_ref, far_ref, hidden_ref,
):
    rows = normalise(other_ref[...], gain_ref[...])
    shared_terms(
        side_ref, rows, flag_ref, gate_ref, up_ref, down_ref, hidden_ref, near_ref, far_ref
    )


def swap4(x):
    return pltpu.roll(x, 4, 1)


def expert_kernel(
    got_ref, gate_hbm, up_hbm, down_hbm, out_hbm,
    gate_ref, up_ref, down_ref, rows_ref, hidden_ref, out_ref, in_sem, sem,
):
    width = 2 * got_ref.shape[2]
    half = width // 2
    hid = gate_ref.shape[0]
    full = EX * MAIN
    quarter = half // 2
    cuts = [(c, min(CUTS[i + 1], hid) - c) for i, c in enumerate(CUTS[:-1])]
    loads = []
    for c, n in cuts:
        cut = pl.ds(c, n)
        loads.append([(gate_hbm.at[cut], gate_ref.at[cut]), (up_hbm.at[cut], up_ref.at[cut])])
    loads.append([(down_hbm, down_ref)])
    count = 0
    for i, group in enumerate(loads):
        for j, (source, target) in enumerate(group):
            group[j] = pltpu.make_async_copy(source, target, in_sem.at[count])
            count += 1

    for group in loads:
        for copy in group:
            copy.start()
    rows_ref[0:full, 0:half] = got_ref[:, 0:MAIN, :].reshape(full, half)
    rows_ref[0:full, half:width] = got_ref[:, MAIN : 2 * MAIN, :].reshape(full, half)
    step = 256
    low = lax.broadcasted_iota(jnp.int32, (EX // 2, 8, step), 1) < REST
    for c in range(0, half, step):
        rest = got_ref[:, 2 * MAIN : BLK, c : c + step].astype(f32).reshape(EX // 2, 2, 8, step)
        even, odd = rest[:, 0], rest[:, 1]
        lo = jnp.where(low, even, swap4(odd))
        hi = jnp.where(low, swap4(even), odd)
        rows_ref[full:, c : c + step] = lo.reshape(EX * REST, step).astype(bf16)
        rows_ref[full:, half + c : half + c + step] = hi.reshape(EX * REST, step).astype(bf16)
    for (c, n), group in zip(cuts, loads):
        for copy in group:
            copy.wait()
        gate = dot_t(rows_ref[...], gate_ref[c : c + n, :])
        up = dot_t(rows_ref[...], up_ref[c : c + n, :])
        hidden_ref[:, c : c + n] = (jax.nn.silu(gate) * up).astype(bf16)
    loads[-1][0].wait()
    low = lax.broadcasted_iota(jnp.int32, (EX // 2, 8, quarter), 1) < REST
    sends = []

    def send(t, first, count):
        rows = pl.ds(first, count)
        copy = pltpu.make_async_copy(
            out_ref.at[:, t, rows, :], out_hbm.at[:, t, rows, :], sem.at[len(sends)]
        )
        copy.start()
        sends.append(copy)

    for t in range(2):
        rests = []
        for h in range(2):
            at = t * half + h * quarter
            part = dot(hidden_ref[...], down_ref[:, at : at + quarter])
            out_ref[:, t, h * MAIN : (h + 1) * MAIN, :] = (
                part[0:full].astype(bf16).reshape(EX, MAIN, quarter)
            )
            if h == 0:
                send(t, 0, MAIN)
            rests.append(part[full:].reshape(EX // 2, 8, quarter))
        lo, hi = rests
        even = jnp.where(low, lo, swap4(hi))
        odd = jnp.where(low, swap4(lo), hi)
        joined = jnp.stack([even, odd], axis=1).reshape(EX, 8, quarter)
        out_ref[:, t, 2 * MAIN : BLK, :] = joined.astype(bf16)
        send(t, MAIN, BLK - MAIN)
    for copy in sends:
        copy.wait()


def combine_kernel(back_ref, main_ref, rest_ref, base_ref, out_ref):
    quarter = back_ref.shape[3]
    lane = lax.broadcasted_iota(jnp.int32, rest_ref.shape, 1)
    for h in range(2):
        mine = (lane % (2 * REST) < REST) == (h == 0)
        few = jnp.where(mine, rest_ref[...].astype(f32), 0.0).astype(bf16)
        total = None
        for t in range(2):
            rows = back_ref[:, t, h * MAIN : (h + 1) * MAIN, :].reshape(EX * MAIN, quarter)
            part = dot(main_ref[...], rows)
            rest = back_ref[:, t, 2 * MAIN : BLK, :].reshape(EX * 2 * REST, quarter)
            part = part + dot(few, rest)
            total = part if total is None else total + part
        cols = slice(h * quarter, (h + 1) * quarter)
        out_ref[:, cols] = (base_ref[:, cols] + total[0:TK] + total[TK:]).astype(bf16)


def call(body, out_shape, **kw):
    mib = kw.pop("mib", 16)
    return pl.pallas_call(
        body, out_shape=out_shape, compiler_params=pltpu.CompilerParams(vmem_limit_bytes=mib << 20), **kw
    )


vmem = pl.BlockSpec(memory_space=pltpu.VMEM)
smem = pl.BlockSpec(memory_space=pltpu.SMEM)
hbm = pl.BlockSpec(memory_space=pl.ANY)


def in_hbm(x):
    return pltpu.with_memory_space_constraint(x, pltpu.HBM)


def in_vmem(x):
    return pltpu.with_memory_space_constraint(x, pltpu.VMEM)


def per_device(
    tokens, norm_gain, router, expert_ids, modality,
    expert_gate, expert_up, expert_down, shared_gate, shared_up, shared_down,
):
    sds = jax.ShapeDtypeStruct
    width = tokens.shape[1]
    half = width // 2
    side = lax.axis_index("tensor").astype(jnp.int32).reshape(1)
    gain = norm_gain.reshape(1, width)
    flags = modality.reshape(1, TK)
    swap = [(0, 1), (1, 0)]
    other_tokens = lax.ppermute(tokens, "dp", swap)
    other_flags = lax.ppermute(flags, "dp", swap)

    outgoing = call(
        place_kernel,
        pltpu.HBM((EX, BLK, half), bf16),
        in_specs=[hbm] * 3,
        out_specs=hbm,
        scratch_shapes=[
            pltpu.VMEM((TK, width), bf16),
            pltpu.VMEM((1, width), f32),
            pltpu.VMEM((expert_ids.shape[1], TK), jnp.int32),
            pltpu.VMEM((EX, BLK, half), bf16),
            pltpu.SemaphoreType.DMA((3,)),
            pltpu.SemaphoreType.DMA((4,)),
        ],
        name="place",
    )(in_hbm(tokens), in_hbm(gain), in_hbm(expert_ids.T))
    got = lax.all_to_all(outgoing, "expert", 0, 0, tiled=True)

    hid = expert_gate.shape[2]
    piece = pltpu.HBM((TK, half), bf16)
    hidden = pltpu.VMEM((2, TK, shared_gate.shape[2]), bf16)
    part = pltpu.VMEM(shared_down.shape, bf16)
    main, rest, own, pair, *weights = call(
        weigh_kernel,
        (
            sds((2 * TK, EX * MAIN), bf16),
            sds((2 * TK, EX * 2 * REST), bf16),
            pltpu.HBM((TK, half), f32),
            piece,
            part,
            part,
            part,
        ),
        in_specs=[smem] + [vmem] * 5 + [hbm] * 3,
        scratch_shapes=[hidden, pltpu.SemaphoreType.DMA((3,))],
        name="weigh",
    )(
        side, tokens, gain, expert_ids.T, router.T, flags,
        in_hbm(shared_gate.swapaxes(1, 2)), in_hbm(shared_up.swapaxes(1, 2)), in_hbm(shared_down),
    )
    four = ("dp", "tensor")
    pair = lax.ppermute(pair, four, [(i, i ^ 1) for i in range(4)])
    near, far = call(
        shared_kernel,
        (piece, piece),
        in_specs=[smem] + [vmem] * 6,
        scratch_shapes=[hidden],
        name="shared",
    )(side, other_tokens, gain, other_flags, *[in_vmem(x) for x in weights])
    near = lax.ppermute(near, four, [(i, i ^ 2) for i in range(4)])
    far = lax.ppermute(far, four, [(i, i ^ 3) for i in range(4)])
    got, main, rest, own, pair, near, far = lax.optimization_barrier(
        (got, main, rest, own, pair, near, far)
    )
    base = own + pair.astype(f32) + near.astype(f32) + far.astype(f32)

    hid = expert_gate.shape[2]
    rows = EX * (MAIN + REST)
    results = call(
        expert_kernel,
        pltpu.HBM((EX, 2, BLK, half // 2), bf16),
        in_specs=[vmem, hbm, hbm, hbm],
        out_specs=hbm,
        scratch_shapes=[
            pltpu.VMEM((hid, width), bf16),
            pltpu.VMEM((hid, width), bf16),
            pltpu.VMEM((hid, width), bf16),
            pltpu.VMEM((rows, width), bf16),
            pltpu.VMEM((rows, hid), bf16),
            pltpu.VMEM((EX, 2, BLK, half // 2), bf16),
            pltpu.SemaphoreType.DMA((2 * len(CUTS) - 1,)),
            pltpu.SemaphoreType.DMA((4,)),
        ],
        mib=32,
        name="expert",
    )(got, in_hbm(expert_gate[0].T), in_hbm(expert_up[0].T), in_hbm(expert_down[0]))
    back = lax.all_to_all(
        results.reshape(2 * EX, BLK, half // 2), ("expert", "tensor"), 0, 0, tiled=True
    ).reshape(EX, 2, BLK, half // 2)
    return call(combine_kernel, sds((TK, half), bf16), name="combine")(back, main, rest, base)


def solution(mesh):
    in_specs = (
        P(("dp", "expert"), None),
        P(),
        P(),
        P(("dp", "expert"), None),
        P(("dp", "expert")),
        P("expert", None, "tensor"),
        P("expert", None, "tensor"),
        P("expert", "tensor", None),
        P(None, None, ("dp", "tensor")),
        P(None, None, ("dp", "tensor")),
        P(None, ("dp", "tensor"), None),
    )
    out_specs = P(("dp", "expert"), "tensor")
    return jax.shard_map(
        per_device, mesh=mesh, in_specs=in_specs, out_specs=out_specs, check_vma=False
    )
```

```python
import functools

import jax
import jax.numpy as jnp
from jax import lax
from jax.experimental import pallas as pl
from jax.experimental.pallas import tpu as pltpu
from jax.sharding import PartitionSpec as P

epsilon = 1e-06
f32 = jnp.float32
bf16 = jnp.bfloat16

EX = 32
TK = 128
MAIN = 16
REST = 4
BLK = 2 * (MAIN + REST)


CUTS = (0, 256, 1 << 20)


def normalise(values, gain):
    values = values.astype(f32)
    inv_scale = lax.rsqrt(jnp.mean(values * values, axis=-1, keepdims=True) + epsilon)
    return (values * inv_scale * gain).astype(bf16)


def dot(a, b):
    return jnp.dot(a, b, preferred_element_type=f32)


def dot_t(a, b):
    return lax.dot_general(a, b, (((1,), (1,)), ((), ())), preferred_element_type=f32)


def slot_ranks(ids):
    expert = lax.broadcasted_iota(jnp.int32, (EX, TK), 0)
    named = ids[0:1] == expert
    for k in range(1, ids.shape[0]):
        named = named | (ids[k : k + 1] == expert)
    ones = jnp.where(named, 1.0, 0.0)
    before = lax.broadcasted_iota(jnp.int32, (TK, TK), 0) < lax.broadcasted_iota(
        jnp.int32, (TK, TK), 1
    )
    rank = dot(ones.astype(bf16), jnp.where(before, 1.0, 0.0).astype(bf16))
    return jnp.where(named, rank, -1.0)


def place_kernel(
    tok_hbm, gain_hbm, ids_hbm, out_hbm, tok_ref, gain_ref, ids_ref, out_ref, sem, out_sem
):
    pairs = ((ids_hbm, ids_ref), (gain_hbm, gain_ref), (tok_hbm, tok_ref))
    copies = [pltpu.make_async_copy(a, b, sem.at[i]) for i, (a, b) in enumerate(pairs)]
    for copy in copies:
        copy.start()
    copies[0].wait()
    rank = slot_ranks(ids_ref[...])
    half = tok_ref.shape[1] // 2
    slot = lax.broadcasted_iota(jnp.int32, (EX, MAIN, TK), 1).astype(f32)
    main = jnp.where(rank[:, None, :] == slot, 1.0, 0.0).astype(bf16).reshape(EX * MAIN, TK)
    row = lax.broadcasted_iota(jnp.int32, (EX, 2 * REST, TK), 1)
    wanted = (row % REST + MAIN).astype(f32)
    rest = jnp.where(rank[:, None, :] == wanted, 1.0, 0.0)
    rest_lo = jnp.where(row < REST, rest, 0.0).astype(bf16).reshape(EX * 2 * REST, TK)
    rest_hi = jnp.where(row >= REST, rest, 0.0).astype(bf16).reshape(EX * 2 * REST, TK)
    rest = jnp.concatenate([rest_lo, rest_hi], axis=1)
    for copy in copies[1:]:
        copy.wait()
    normed = normalise(tok_ref[...], gain_ref[...])
    step = 256
    sends = []
    for c in range(0, half, step):
        lo = normed[:, c : c + step]
        hi = normed[:, half + c : half + c + step]
        out_ref[:, 0:MAIN, c : c + step] = dot(main, lo).astype(bf16).reshape(EX, MAIN, step)
        out_ref[:, MAIN : 2 * MAIN, c : c + step] = (
            dot(main, hi).astype(bf16).reshape(EX, MAIN, step)
        )
        both = dot(rest, jnp.concatenate([lo, hi], axis=0))
        out_ref[:, 2 * MAIN : BLK, c : c + step] = both.reshape(EX, 2 * REST, step).astype(bf16)
        cols = pl.ds(c, step)
        send = pltpu.make_async_copy(
            out_ref.at[:, :, cols], out_hbm.at[:, :, cols], out_sem.at[len(sends)]
        )
        send.start()
        sends.append(send)
    for send in sends:
        send.wait()


def weigh_kernel(
    side_ref, tok_ref, gain_ref, ids_ref, router_ref, flag_ref, gate_hbm, up_hbm, down_hbm,
    main_ref, rest_ref, own_ref, pair_ref, gate_ref, up_ref, down_ref, hidden_ref, sem,
):
    pairs = ((gate_hbm, gate_ref), (up_hbm, up_ref), (down_hbm, down_ref))
    copies = [pltpu.make_async_copy(a, b, sem.at[i]) for i, (a, b) in enumerate(pairs)]
    for copy in copies:
        copy.start()
    rank = slot_ranks(ids_ref[...])
    normed = normalise(tok_ref[...], gain_ref[...])
    logits = dot_t(router_ref[...], normed)
    scores = jnp.where(rank >= 0.0, jax.nn.sigmoid(logits), 0.0)
    weights = scores / jnp.sum(scores, axis=0, keepdims=True)
    slot = lax.broadcasted_iota(jnp.int32, (EX, MAIN, TK), 1).astype(f32)
    main = jnp.where(rank[:, None, :] == slot, weights[:, None, :], 0.0)
    main_ref[...] = main.reshape(EX * MAIN, TK).T.astype(bf16)
    row = lax.broadcasted_iota(jnp.int32, (EX, 2 * REST, TK), 1)
    wanted = (row % REST + MAIN).astype(f32)
    rest = jnp.where(rank[:, None, :] == wanted, weights[:, None, :], 0.0)
    rest_ref[...] = rest.reshape(EX * 2 * REST, TK).T.astype(bf16)
    for copy in copies:
        copy.wait()
    shared_terms(
        side_ref, normed, flag_ref, gate_ref, up_ref, down_ref, hidden_ref,
        own_ref, pair_ref,
    )


def shared_terms(
    side_ref, rows, flag_ref, gate_ref, up_ref, down_ref, hidden_ref, same_ref, cross_ref
):
    flag = jnp.broadcast_to(flag_ref[...].astype(f32), (TK, TK)).T[:, 0:1]
    for m in range(gate_ref.shape[0]):
        keep = flag if m == 0 else 1.0 - flag
        gate = dot_t(rows, gate_ref[m])
        up = dot_t(rows, up_ref[m])
        hidden_ref[m] = (jax.nn.silu(gate) * up * keep).astype(bf16)
    side = side_ref[0]
    half = same_ref.shape[1]
    for target, at in ((cross_ref, 1 - side), (same_ref, side)):
        cols = pl.ds(pl.multiple_of(at * half, half), half)
        part = dot(hidden_ref[0], down_ref[0, :, cols])
        part = part + dot(hidden_ref[1], down_ref[1, :, cols])
        target[...] = part.astype(target.dtype)


def shared_kernel(
    side_ref, other_ref, gain_ref, flag_ref, gate_ref, up_ref, down_ref,
    near_ref, far_ref, hidden_ref,
):
    rows = normalise(other_ref[...], gain_ref[...])
    shared_terms(
        side_ref, rows, flag_ref, gate_ref, up_ref, down_ref, hidden_ref, near_ref, far_ref
    )


def swap4(x):
    return pltpu.roll(x, 4, 1)


def expert_kernel(
    got_ref, gate_hbm, up_hbm, down_hbm, out_hbm,
    gate_ref, up_ref, down_ref, rows_ref, hidden_ref, out_ref, in_sem, sem,
):
    width = 2 * got_ref.shape[2]
    half = width // 2
    hid = gate_ref.shape[0]
    full = EX * MAIN
    quarter = half // 2
    cuts = [(c, min(CUTS[i + 1], hid) - c) for i, c in enumerate(CUTS[:-1])]
    loads = []
    for c, n in cuts:
        cut = pl.ds(c, n)
        loads.append([(gate_hbm.at[cut], gate_ref.at[cut]), (up_hbm.at[cut], up_ref.at[cut])])
    loads.append([(down_hbm, down_ref)])
    count = 0
    for i, group in enumerate(loads):
        for j, (source, target) in enumerate(group):
            group[j] = pltpu.make_async_copy(source, target, in_sem.at[count])
            count += 1

    for group in loads:
        for copy in group:
            copy.start()
    rows_ref[0:full, 0:half] = got_ref[:, 0:MAIN, :].reshape(full, half)
    rows_ref[0:full, half:width] = got_ref[:, MAIN : 2 * MAIN, :].reshape(full, half)
    step = 256
    low = lax.broadcasted_iota(jnp.int32, (EX // 2, 8, step), 1) < REST
    for c in range(0, half, step):
        rest = got_ref[:, 2 * MAIN : BLK, c : c + step].astype(f32).reshape(EX // 2, 2, 8, step)
        even, odd = rest[:, 0], rest[:, 1]
        lo = jnp.where(low, even, swap4(odd))
        hi = jnp.where(low, swap4(even), odd)
        rows_ref[full:, c : c + step] = lo.reshape(EX * REST, step).astype(bf16)
        rows_ref[full:, half + c : half + c + step] = hi.reshape(EX * REST, step).astype(bf16)
    for (c, n), group in zip(cuts, loads):
        for copy in group:
            copy.wait()
        gate = dot_t(rows_ref[...], gate_ref[c : c + n, :])
        up = dot_t(rows_ref[...], up_ref[c : c + n, :])
        hidden_ref[:, c : c + n] = (jax.nn.silu(gate) * up).astype(bf16)
    loads[-1][0].wait()
    low = lax.broadcasted_iota(jnp.int32, (EX // 2, 8, quarter), 1) < REST
    sends = []

    def send(t, first, count):
        rows = pl.ds(first, count)
        copy = pltpu.make_async_copy(
            out_ref.at[:, t, rows, :], out_hbm.at[:, t, rows, :], sem.at[len(sends)]
        )
        copy.start()
        sends.append(copy)

    for t in range(2):
        rests = []
        for h in range(2):
            at = t * half + h * quarter
            part = dot(hidden_ref[...], down_ref[:, at : at + quarter])
            out_ref[:, t, h * MAIN : (h + 1) * MAIN, :] = (
                part[0:full].astype(bf16).reshape(EX, MAIN, quarter)
            )
            if h == 0:
                send(t, 0, MAIN)
            rests.append(part[full:].reshape(EX // 2, 8, quarter))
        lo, hi = rests
        even = jnp.where(low, lo, swap4(hi))
        odd = jnp.where(low, swap4(lo), hi)
        joined = jnp.stack([even, odd], axis=1).reshape(EX, 8, quarter)
        out_ref[:, t, 2 * MAIN : BLK, :] = joined.astype(bf16)
        send(t, MAIN, BLK - MAIN)
    for copy in sends:
        copy.wait()


def combine_kernel(back_ref, main_ref, rest_ref, base_ref, out_ref):
    quarter = back_ref.shape[3]
    lane = lax.broadcasted_iota(jnp.int32, rest_ref.shape, 1)
    for h in range(2):
        mine = (lane % (2 * REST) < REST) == (h == 0)
        few = jnp.where(mine, rest_ref[...].astype(f32), 0.0).astype(bf16)
        total = None
        for t in range(2):
            rows = back_ref[:, t, h * MAIN : (h + 1) * MAIN, :].reshape(EX * MAIN, quarter)
            part = dot(main_ref[...], rows)
            rest = back_ref[:, t, 2 * MAIN : BLK, :].reshape(EX * 2 * REST, quarter)
            part = part + dot(few, rest)
            total = part if total is None else total + part
        cols = slice(h * quarter, (h + 1) * quarter)
        out_ref[:, cols] = (base_ref[:, cols] + total).astype(bf16)


def call(body, out_shape, **kw):
    mib = kw.pop("mib", 16)
    return pl.pallas_call(
        body, out_shape=out_shape, compiler_params=pltpu.CompilerParams(vmem_limit_bytes=mib << 20), **kw
    )


vmem = pl.BlockSpec(memory_space=pltpu.VMEM)
smem = pl.BlockSpec(memory_space=pltpu.SMEM)
hbm = pl.BlockSpec(memory_space=pl.ANY)


def in_hbm(x):
    return pltpu.with_memory_space_constraint(x, pltpu.HBM)


def in_vmem(x):
    return pltpu.with_memory_space_constraint(x, pltpu.VMEM)


def per_device(
    tokens, norm_gain, router, expert_ids, modality,
    expert_gate, expert_up, expert_down, shared_gate, shared_up, shared_down,
):
    sds = jax.ShapeDtypeStruct
    width = tokens.shape[1]
    half = width // 2
    side = lax.axis_index("tensor").astype(jnp.int32).reshape(1)
    gain = norm_gain.reshape(1, width)
    flags = modality.reshape(1, TK)
    swap = [(0, 1), (1, 0)]
    other_tokens = lax.ppermute(tokens, "dp", swap)
    other_flags = lax.ppermute(flags, "dp", swap)

    outgoing = call(
        place_kernel,
        pltpu.HBM((EX, BLK, half), bf16),
        in_specs=[hbm] * 3,
        out_specs=hbm,
        scratch_shapes=[
            pltpu.VMEM((TK, width), bf16),
            pltpu.VMEM((1, width), f32),
            pltpu.VMEM((expert_ids.shape[1], TK), jnp.int32),
            pltpu.VMEM((EX, BLK, half), bf16),
            pltpu.SemaphoreType.DMA((3,)),
            pltpu.SemaphoreType.DMA((4,)),
        ],
        name="place",
    )(in_hbm(tokens), in_hbm(gain), in_hbm(expert_ids.T))
    got = lax.all_to_all(outgoing, "expert", 0, 0, tiled=True)

    hid = expert_gate.shape[2]
    piece = pltpu.HBM((TK, half), bf16)
    hidden = pltpu.VMEM((2, TK, shared_gate.shape[2]), bf16)
    part = pltpu.VMEM(shared_down.shape, bf16)
    main, rest, own, pair, *weights = call(
        weigh_kernel,
        (
            sds((TK, EX * MAIN), bf16),
            sds((TK, EX * 2 * REST), bf16),
            pltpu.HBM((TK, half), f32),
            piece,
            part,
            part,
            part,
        ),
        in_specs=[smem] + [vmem] * 5 + [hbm] * 3,
        scratch_shapes=[hidden, pltpu.SemaphoreType.DMA((3,))],
        name="weigh",
    )(
        side, tokens, gain, expert_ids.T, router.T, flags,
        in_hbm(shared_gate.swapaxes(1, 2)), in_hbm(shared_up.swapaxes(1, 2)), in_hbm(shared_down),
    )
    four = ("dp", "tensor")
    pair = lax.ppermute(pair, four, [(i, i ^ 1) for i in range(4)])
    near, far = call(
        shared_kernel,
        (piece, piece),
        in_specs=[smem] + [vmem] * 6,
        scratch_shapes=[hidden],
        name="shared",
    )(side, other_tokens, gain, other_flags, *[in_vmem(x) for x in weights])
    near = lax.ppermute(near, four, [(i, i ^ 2) for i in range(4)])
    far = lax.ppermute(far, four, [(i, i ^ 3) for i in range(4)])
    got, main, rest, own, pair, near, far = lax.optimization_barrier(
        (got, main, rest, own, pair, near, far)
    )
    base = own + pair.astype(f32) + near.astype(f32) + far.astype(f32)

    hid = expert_gate.shape[2]
    rows = EX * (MAIN + REST)
    results = call(
        expert_kernel,
        pltpu.HBM((EX, 2, BLK, half // 2), bf16),
        in_specs=[vmem, hbm, hbm, hbm],
        out_specs=hbm,
        scratch_shapes=[
            pltpu.VMEM((hid, width), bf16),
            pltpu.VMEM((hid, width), bf16),
            pltpu.VMEM((hid, width), bf16),
            pltpu.VMEM((rows, width), bf16),
            pltpu.VMEM((rows, hid), bf16),
            pltpu.VMEM((EX, 2, BLK, half // 2), bf16),
            pltpu.SemaphoreType.DMA((2 * len(CUTS) - 1,)),
            pltpu.SemaphoreType.DMA((4,)),
        ],
        mib=32,
        name="expert",
    )(got, in_hbm(expert_gate[0].T), in_hbm(expert_up[0].T), in_hbm(expert_down[0]))
    back = lax.all_to_all(
        results.reshape(2 * EX, BLK, half // 2), ("expert", "tensor"), 0, 0, tiled=True
    ).reshape(EX, 2, BLK, half // 2)
    return call(combine_kernel, sds((TK, half), bf16), name="combine")(back, main, rest, base)


def solution(mesh):
    in_specs = (
        P(("dp", "expert"), None),
        P(),
        P(),
        P(("dp", "expert"), None),
        P(("dp", "expert")),
        P("expert", None, "tensor"),
        P("expert", None, "tensor"),
        P("expert", "tensor", None),
        P(None, None, ("dp", "tensor")),
        P(None, None, ("dp", "tensor")),
        P(None, ("dp", "tensor"), None),
    )
    out_specs = P(("dp", "expert"), "tensor")
    return jax.shard_map(
        per_device, mesh=mesh, in_specs=in_specs, out_specs=out_specs, check_vma=False
    )
```

```python
import functools

import jax
import jax.numpy as jnp
from jax import lax
from jax.experimental import pallas as pl
from jax.experimental.pallas import tpu as pltpu
from jax.sharding import PartitionSpec as P

epsilon = 1e-06
f32 = jnp.float32
bf16 = jnp.bfloat16

EX = 32
TK = 128
MAIN = 16
REST = 4
BLK = 2 * (MAIN + REST)


CUTS = (0, 320, 1 << 20)


def normalise(values, gain):
    values = values.astype(f32)
    inv_scale = lax.rsqrt(jnp.mean(values * values, axis=-1, keepdims=True) + epsilon)
    return (values * inv_scale * gain).astype(bf16)


def dot(a, b):
    return jnp.dot(a, b, preferred_element_type=f32)


def dot_t(a, b):
    return lax.dot_general(a, b, (((1,), (1,)), ((), ())), preferred_element_type=f32)


def slot_ranks(ids):
    expert = lax.broadcasted_iota(jnp.int32, (EX, TK), 0)
    named = ids[0:1] == expert
    for k in range(1, ids.shape[0]):
        named = named | (ids[k : k + 1] == expert)
    ones = jnp.where(named, 1.0, 0.0)
    before = lax.broadcasted_iota(jnp.int32, (TK, TK), 0) < lax.broadcasted_iota(
        jnp.int32, (TK, TK), 1
    )
    rank = dot(ones.astype(bf16), jnp.where(before, 1.0, 0.0).astype(bf16))
    return jnp.where(named, rank, -1.0)


def place_kernel(
    tok_hbm, gain_hbm, ids_hbm, out_hbm, tok_ref, gain_ref, ids_ref, out_ref, sem, out_sem
):
    pairs = ((ids_hbm, ids_ref), (gain_hbm, gain_ref), (tok_hbm, tok_ref))
    copies = [pltpu.make_async_copy(a, b, sem.at[i]) for i, (a, b) in enumerate(pairs)]
    for copy in copies:
        copy.start()
    copies[0].wait()
    rank = slot_ranks(ids_ref[...])
    half = tok_ref.shape[1] // 2
    slot = lax.broadcasted_iota(jnp.int32, (EX, MAIN, TK), 1).astype(f32)
    main = jnp.where(rank[:, None, :] == slot, 1.0, 0.0).astype(bf16).reshape(EX * MAIN, TK)
    row = lax.broadcasted_iota(jnp.int32, (EX, 2 * REST, TK), 1)
    wanted = (row % REST + MAIN).astype(f32)
    rest = jnp.where(rank[:, None, :] == wanted, 1.0, 0.0)
    rest_lo = jnp.where(row < REST, rest, 0.0).astype(bf16).reshape(EX * 2 * REST, TK)
    rest_hi = jnp.where(row >= REST, rest, 0.0).astype(bf16).reshape(EX * 2 * REST, TK)
    rest = jnp.concatenate([rest_lo, rest_hi], axis=1)
    for copy in copies[1:]:
        copy.wait()
    normed = normalise(tok_ref[...], gain_ref[...])
    sends = []
    edges = [half * i // 8 for i in (0, 2, 4, 6, 7, 8)]
    for c, end in zip(edges, edges[1:]):
        step = end - c
        lo = normed[:, c : c + step]
        hi = normed[:, half + c : half + c + step]
        out_ref[:, 0:MAIN, c : c + step] = dot(main, lo).astype(bf16).reshape(EX, MAIN, step)
        out_ref[:, MAIN : 2 * MAIN, c : c + step] = (
            dot(main, hi).astype(bf16).reshape(EX, MAIN, step)
        )
        both = dot(rest, jnp.concatenate([lo, hi], axis=0))
        out_ref[:, 2 * MAIN : BLK, c : c + step] = both.reshape(EX, 2 * REST, step).astype(bf16)
        cols = pl.ds(c, step)
        send = pltpu.make_async_copy(
            out_ref.at[:, :, cols], out_hbm.at[:, :, cols], out_sem.at[len(sends)]
        )
        send.start()
        sends.append(send)
    for send in sends:
        send.wait()


def weigh_kernel(
    side_ref, tok_ref, gain_ref, ids_ref, router_ref, flag_ref, gate_hbm, up_hbm, down_hbm,
    main_ref, rest_ref, own_ref, pair_ref, gate_ref, up_ref, down_ref, hidden_ref, sem,
):
    pairs = ((gate_hbm, gate_ref), (up_hbm, up_ref), (down_hbm, down_ref))
    copies = [pltpu.make_async_copy(a, b, sem.at[i]) for i, (a, b) in enumerate(pairs)]
    for copy in copies:
        copy.start()
    rank = slot_ranks(ids_ref[...])
    normed = normalise(tok_ref[...], gain_ref[...])
    logits = dot_t(router_ref[...], normed)
    scores = jnp.where(rank >= 0.0, jax.nn.sigmoid(logits), 0.0)
    weights = scores / jnp.sum(scores, axis=0, keepdims=True)
    slot = lax.broadcasted_iota(jnp.int32, (EX, MAIN, TK), 1).astype(f32)
    main = jnp.where(rank[:, None, :] == slot, weights[:, None, :], 0.0)
    main_ref[...] = main.reshape(EX * MAIN, TK).T.astype(bf16)
    row = lax.broadcasted_iota(jnp.int32, (EX, 2 * REST, TK), 1)
    wanted = (row % REST + MAIN).astype(f32)
    rest = jnp.where(rank[:, None, :] == wanted, weights[:, None, :], 0.0)
    for h in range(2):
        part = jnp.where((row < REST) == (h == 0), rest, 0.0)
        rest_ref[h] = part.reshape(EX * 2 * REST, TK).T.astype(bf16)
    for copy in copies:
        copy.wait()
    shared_terms(
        side_ref, normed, flag_ref, gate_ref, up_ref, down_ref, hidden_ref,
        own_ref, pair_ref,
    )


def shared_terms(
    side_ref, rows, flag_ref, gate_ref, up_ref, down_ref, hidden_ref, same_ref, cross_ref
):
    flag = jnp.broadcast_to(flag_ref[...].astype(f32), (TK, TK)).T[:, 0:1]
    for m in range(gate_ref.shape[0]):
        keep = flag if m == 0 else 1.0 - flag
        gate = dot_t(rows, gate_ref[m])
        up = dot_t(rows, up_ref[m])
        hidden_ref[m] = (jax.nn.silu(gate) * up * keep).astype(bf16)
    side = side_ref[0]
    half = same_ref.shape[1]
    for target, at in ((cross_ref, 1 - side), (same_ref, side)):
        cols = pl.ds(pl.multiple_of(at * half, half), half)
        part = dot(hidden_ref[0], down_ref[0, :, cols])
        part = part + dot(hidden_ref[1], down_ref[1, :, cols])
        target[...] = part.astype(target.dtype)


def shared_kernel(
    side_ref, other_ref, gain_ref, flag_ref, gate_ref, up_ref, down_ref,
    near_ref, far_ref, hidden_ref,
):
    rows = normalise(other_ref[...], gain_ref[...])
    shared_terms(
        side_ref, rows, flag_ref, gate_ref, up_ref, down_ref, hidden_ref, near_ref, far_ref
    )


def swap4(x):
    return pltpu.roll(x, 4, 1)


def expert_kernel(
    got_ref, gate_hbm, up_hbm, down_hbm, out_hbm,
    gate_ref, up_ref, down_ref, rows_ref, hidden_ref, out_ref, in_sem, sem,
):
    width = 2 * got_ref.shape[2]
    half = width // 2
    hid = gate_ref.shape[0]
    full = EX * MAIN
    quarter = half // 2
    cuts = [(c, min(CUTS[i + 1], hid) - c) for i, c in enumerate(CUTS[:-1])]
    loads = []
    for c, n in cuts:
        cut = pl.ds(c, n)
        loads.append([(gate_hbm.at[cut], gate_ref.at[cut]), (up_hbm.at[cut], up_ref.at[cut])])
    loads.append([(down_hbm, down_ref)])
    count = 0
    for i, group in enumerate(loads):
        for j, (source, target) in enumerate(group):
            group[j] = pltpu.make_async_copy(source, target, in_sem.at[count])
            count += 1

    for group in loads:
        for copy in group:
            copy.start()
    rows_ref[0:full, 0:half] = got_ref[:, 0:MAIN, :].reshape(full, half)
    rows_ref[0:full, half:width] = got_ref[:, MAIN : 2 * MAIN, :].reshape(full, half)
    step = 256
    low = lax.broadcasted_iota(jnp.int32, (EX // 2, 8, step), 1) < REST
    for c in range(0, half, step):
        rest = got_ref[:, 2 * MAIN : BLK, c : c + step].astype(f32).reshape(EX // 2, 2, 8, step)
        even, odd = rest[:, 0], rest[:, 1]
        lo = jnp.where(low, even, swap4(odd))
        hi = jnp.where(low, swap4(even), odd)
        rows_ref[full:, c : c + step] = lo.reshape(EX * REST, step).astype(bf16)
        rows_ref[full:, half + c : half + c + step] = hi.reshape(EX * REST, step).astype(bf16)
    for (c, n), group in zip(cuts, loads):
        for copy in group:
            copy.wait()
        gate = dot_t(rows_ref[...], gate_ref[c : c + n, :])
        up = dot_t(rows_ref[...], up_ref[c : c + n, :])
        hidden_ref[:, c : c + n] = (jax.nn.silu(gate) * up).astype(bf16)
    loads[-1][0].wait()
    low = lax.broadcasted_iota(jnp.int32, (EX // 2, 8, quarter), 1) < REST
    sends = []

    def send(t, first, count):
        rows = pl.ds(first, count)
        copy = pltpu.make_async_copy(
            out_ref.at[:, t, rows, :], out_hbm.at[:, t, rows, :], sem.at[len(sends)]
        )
        copy.start()
        sends.append(copy)

    for t in range(2):
        rests = []
        for h in range(2):
            at = t * half + h * quarter
            part = dot(hidden_ref[...], down_ref[:, at : at + quarter])
            out_ref[:, t, h * MAIN : (h + 1) * MAIN, :] = (
                part[0:full].astype(bf16).reshape(EX, MAIN, quarter)
            )
            if h == 0:
                send(t, 0, MAIN)
            rests.append(part[full:].reshape(EX // 2, 8, quarter))
        lo, hi = rests
        even = jnp.where(low, lo, swap4(hi))
        odd = jnp.where(low, swap4(lo), hi)
        joined = jnp.stack([even, odd], axis=1).reshape(EX, 8, quarter)
        out_ref[:, t, 2 * MAIN : BLK, :] = joined.astype(bf16)
        send(t, MAIN, BLK - MAIN)
    for copy in sends:
        copy.wait()


def combine_kernel(back_ref, main_ref, rest_ref, base_ref, out_ref):
    quarter = back_ref.shape[3]
    for h in range(2):
        total = None
        for t in range(2):
            rows = back_ref[:, t, h * MAIN : (h + 1) * MAIN, :].reshape(EX * MAIN, quarter)
            part = dot(main_ref[...], rows)
            rest = back_ref[:, t, 2 * MAIN : BLK, :].reshape(EX * 2 * REST, quarter)
            part = part + dot(rest_ref[h], rest)
            total = part if total is None else total + part
        cols = slice(h * quarter, (h + 1) * quarter)
        out_ref[:, cols] = (base_ref[:, cols] + total).astype(bf16)


def call(body, out_shape, **kw):
    mib = kw.pop("mib", 16)
    return pl.pallas_call(
        body, out_shape=out_shape, compiler_params=pltpu.CompilerParams(vmem_limit_bytes=mib << 20), **kw
    )


vmem = pl.BlockSpec(memory_space=pltpu.VMEM)
smem = pl.BlockSpec(memory_space=pltpu.SMEM)
hbm = pl.BlockSpec(memory_space=pl.ANY)


def in_hbm(x):
    return pltpu.with_memory_space_constraint(x, pltpu.HBM)


def in_vmem(x):
    return pltpu.with_memory_space_constraint(x, pltpu.VMEM)


def per_device(
    tokens, norm_gain, router, expert_ids, modality,
    expert_gate, expert_up, expert_down, shared_gate, shared_up, shared_down,
):
    sds = jax.ShapeDtypeStruct
    width = tokens.shape[1]
    half = width // 2
    side = lax.axis_index("tensor").astype(jnp.int32).reshape(1)
    gain = norm_gain.reshape(1, width)
    flags = modality.reshape(1, TK)
    swap = [(0, 1), (1, 0)]
    other_tokens = lax.ppermute(tokens, "dp", swap)
    other_flags = lax.ppermute(flags, "dp", swap)

    outgoing = call(
        place_kernel,
        pltpu.HBM((EX, BLK, half), bf16),
        in_specs=[hbm] * 3,
        out_specs=hbm,
        scratch_shapes=[
            pltpu.VMEM((TK, width), bf16),
            pltpu.VMEM((1, width), f32),
            pltpu.VMEM((expert_ids.shape[1], TK), jnp.int32),
            pltpu.VMEM((EX, BLK, half), bf16),
            pltpu.SemaphoreType.DMA((3,)),
            pltpu.SemaphoreType.DMA((5,)),
        ],
        name="place",
    )(in_hbm(tokens), in_hbm(gain), in_hbm(expert_ids.T))
    got = lax.all_to_all(outgoing, "expert", 0, 0, tiled=True)

    hid = expert_gate.shape[2]
    piece = pltpu.HBM((TK, half), bf16)
    hidden = pltpu.VMEM((2, TK, shared_gate.shape[2]), bf16)
    part = pltpu.VMEM(shared_down.shape, bf16)
    main, rest, own, pair, *weights = call(
        weigh_kernel,
        (
            sds((TK, EX * MAIN), bf16),
            sds((2, TK, EX * 2 * REST), bf16),
            pltpu.HBM((TK, half), f32),
            piece,
            part,
            part,
            part,
        ),
        in_specs=[smem] + [vmem] * 5 + [hbm] * 3,
        scratch_shapes=[hidden, pltpu.SemaphoreType.DMA((3,))],
        name="weigh",
    )(
        side, tokens, gain, expert_ids.T, router.T, flags,
        in_hbm(shared_gate.swapaxes(1, 2)), in_hbm(shared_up.swapaxes(1, 2)), in_hbm(shared_down),
    )
    four = ("dp", "tensor")
    pair = lax.ppermute(pair, four, [(i, i ^ 1) for i in range(4)])
    near, far = call(
        shared_kernel,
        (piece, piece),
        in_specs=[smem] + [vmem] * 6,
        scratch_shapes=[hidden],
        name="shared",
    )(side, other_tokens, gain, other_flags, *[in_vmem(x) for x in weights])
    near = lax.ppermute(near, four, [(i, i ^ 2) for i in range(4)])
    far = lax.ppermute(far, four, [(i, i ^ 3) for i in range(4)])
    got, main, rest, own, pair, near, far = lax.optimization_barrier(
        (got, main, rest, own, pair, near, far)
    )
    base = own + pair.astype(f32) + near.astype(f32) + far.astype(f32)

    hid = expert_gate.shape[2]
    rows = EX * (MAIN + REST)
    results = call(
        expert_kernel,
        pltpu.HBM((EX, 2, BLK, half // 2), bf16),
        in_specs=[vmem, hbm, hbm, hbm],
        out_specs=hbm,
        scratch_shapes=[
            pltpu.VMEM((hid, width), bf16),
            pltpu.VMEM((hid, width), bf16),
            pltpu.VMEM((hid, width), bf16),
            pltpu.VMEM((rows, width), bf16),
            pltpu.VMEM((rows, hid), bf16),
            pltpu.VMEM((EX, 2, BLK, half // 2), bf16),
            pltpu.SemaphoreType.DMA((2 * len(CUTS) - 1,)),
            pltpu.SemaphoreType.DMA((4,)),
        ],
        mib=32,
        name="expert",
    )(got, in_hbm(expert_gate[0].T), in_hbm(expert_up[0].T), in_hbm(expert_down[0]))
    back = lax.all_to_all(
        results.reshape(2 * EX, BLK, half // 2), ("expert", "tensor"), 0, 0, tiled=True
    ).reshape(EX, 2, BLK, half // 2)
    return call(combine_kernel, sds((TK, half), bf16), name="combine")(back, main, rest, base)


def solution(mesh):
    in_specs = (
        P(("dp", "expert"), None),
        P(),
        P(),
        P(("dp", "expert"), None),
        P(("dp", "expert")),
        P("expert", None, "tensor"),
        P("expert", None, "tensor"),
        P("expert", "tensor", None),
        P(None, None, ("dp", "tensor")),
        P(None, None, ("dp", "tensor")),
        P(None, ("dp", "tensor"), None),
    )
    out_specs = P(("dp", "expert"), "tensor")
    return jax.shard_map(
        per_device, mesh=mesh, in_specs=in_specs, out_specs=out_specs, check_vma=False
    )
```

```python
import functools

import jax
import jax.numpy as jnp
from jax import lax
from jax.experimental import pallas as pl
from jax.experimental.pallas import tpu as pltpu
from jax.sharding import PartitionSpec as P

epsilon = 1e-06
f32 = jnp.float32
bf16 = jnp.bfloat16

EX = 32
TK = 128
MAIN = 16
REST = 4
BLK = 2 * (MAIN + REST)


CUTS = (0, 256, 1 << 20)


def normalise(values, gain):
    values = values.astype(f32)
    inv_scale = lax.rsqrt(jnp.mean(values * values, axis=-1, keepdims=True) + epsilon)
    return (values * inv_scale * gain).astype(bf16)


def dot(a, b):
    return jnp.dot(a, b, preferred_element_type=f32)


def dot_t(a, b):
    return lax.dot_general(a, b, (((1,), (1,)), ((), ())), preferred_element_type=f32)


def slot_ranks(ids):
    expert = lax.broadcasted_iota(jnp.int32, (EX, TK), 0)
    named = ids[0:1] == expert
    for k in range(1, ids.shape[0]):
        named = named | (ids[k : k + 1] == expert)
    ones = jnp.where(named, 1.0, 0.0)
    before = lax.broadcasted_iota(jnp.int32, (TK, TK), 0) < lax.broadcasted_iota(
        jnp.int32, (TK, TK), 1
    )
    rank = dot(ones.astype(bf16), jnp.where(before, 1.0, 0.0).astype(bf16))
    return jnp.where(named, rank, -1.0)


def place_kernel(
    tok_hbm, gain_hbm, ids_hbm, out_hbm, tok_ref, gain_ref, ids_ref, out_ref, sem, out_sem
):
    pairs = ((ids_hbm, ids_ref), (gain_hbm, gain_ref), (tok_hbm, tok_ref))
    copies = [pltpu.make_async_copy(a, b, sem.at[i]) for i, (a, b) in enumerate(pairs)]
    for copy in copies:
        copy.start()
    copies[0].wait()
    rank = slot_ranks(ids_ref[...])
    half = tok_ref.shape[1] // 2
    slot = lax.broadcasted_iota(jnp.int32, (EX, MAIN, TK), 1).astype(f32)
    main = jnp.where(rank[:, None, :] == slot, 1.0, 0.0).astype(bf16).reshape(EX * MAIN, TK)
    row = lax.broadcasted_iota(jnp.int32, (EX, 2 * REST, TK), 1)
    wanted = (row % REST + MAIN).astype(f32)
    rest = jnp.where(rank[:, None, :] == wanted, 1.0, 0.0)
    rest_lo = jnp.where(row < REST, rest, 0.0).astype(bf16).reshape(EX * 2 * REST, TK)
    rest_hi = jnp.where(row >= REST, rest, 0.0).astype(bf16).reshape(EX * 2 * REST, TK)
    rest = jnp.concatenate([rest_lo, rest_hi], axis=1)
    for copy in copies[1:]:
        copy.wait()
    normed = normalise(tok_ref[...], gain_ref[...])
    step = 256
    sends = []
    for c in range(0, half, step):
        lo = normed[:, c : c + step]
        hi = normed[:, half + c : half + c + step]
        out_ref[:, 0:MAIN, c : c + step] = dot(main, lo).astype(bf16).reshape(EX, MAIN, step)
        out_ref[:, MAIN : 2 * MAIN, c : c + step] = (
            dot(main, hi).astype(bf16).reshape(EX, MAIN, step)
        )
        both = dot(rest, jnp.concatenate([lo, hi], axis=0))
        out_ref[:, 2 * MAIN : BLK, c : c + step] = both.reshape(EX, 2 * REST, step).astype(bf16)
        cols = pl.ds(c, step)
        send = pltpu.make_async_copy(
            out_ref.at[:, :, cols], out_hbm.at[:, :, cols], out_sem.at[len(sends)]
        )
        send.start()
        sends.append(send)
    for send in sends:
        send.wait()


def weigh_kernel(
    side_ref, tok_ref, gain_ref, ids_ref, router_ref, flag_ref, gate_hbm, up_hbm, down_hbm,
    main_ref, rest_ref, own_ref, pair_ref, gate_ref, up_ref, down_ref, hidden_ref, sem,
):
    pairs = ((gate_hbm, gate_ref), (up_hbm, up_ref), (down_hbm, down_ref))
    copies = [pltpu.make_async_copy(a, b, sem.at[i]) for i, (a, b) in enumerate(pairs)]
    for copy in copies:
        copy.start()
    rank = slot_ranks(ids_ref[...])
    normed = normalise(tok_ref[...], gain_ref[...])
    logits = dot_t(router_ref[...], normed)
    scores = jnp.where(rank >= 0.0, jax.nn.sigmoid(logits), 0.0)
    weights = scores / jnp.sum(scores, axis=0, keepdims=True)
    slot = lax.broadcasted_iota(jnp.int32, (EX, MAIN, TK), 1).astype(f32)
    main = jnp.where(rank[:, None, :] == slot, weights[:, None, :], 0.0)
    main_ref[...] = main.reshape(EX * MAIN, TK).T.astype(bf16)
    row = lax.broadcasted_iota(jnp.int32, (EX, 2 * REST, TK), 1)
    wanted = (row % REST + MAIN).astype(f32)
    rest = jnp.where(rank[:, None, :] == wanted, weights[:, None, :], 0.0)
    rest_ref[...] = rest.reshape(EX * 2 * REST, TK).T.astype(bf16)
    for copy in copies:
        copy.wait()
    shared_terms(
        side_ref, normed, flag_ref, gate_ref, up_ref, down_ref, hidden_ref,
        own_ref, pair_ref,
    )


def shared_terms(
    side_ref, rows, flag_ref, gate_ref, up_ref, down_ref, hidden_ref, same_ref, cross_ref
):
    flag = jnp.broadcast_to(flag_ref[...].astype(f32), (TK, TK)).T[:, 0:1]
    for m in range(gate_ref.shape[0]):
        keep = flag if m == 0 else 1.0 - flag
        gate = dot_t(rows, gate_ref[m])
        up = dot_t(rows, up_ref[m])
        hidden_ref[m] = (jax.nn.silu(gate) * up * keep).astype(bf16)
    side = side_ref[0]
    half = same_ref.shape[1]
    for target, at in ((cross_ref, 1 - side), (same_ref, side)):
        cols = pl.ds(pl.multiple_of(at * half, half), half)
        part = dot(hidden_ref[0], down_ref[0, :, cols])
        part = part + dot(hidden_ref[1], down_ref[1, :, cols])
        target[...] = part.astype(target.dtype)


def shared_kernel(
    side_ref, other_ref, gain_ref, flag_ref, gate_ref, up_ref, down_ref,
    near_ref, far_ref, hidden_ref,
):
    rows = normalise(other_ref[...], gain_ref[...])
    shared_terms(
        side_ref, rows, flag_ref, gate_ref, up_ref, down_ref, hidden_ref, near_ref, far_ref
    )


def swap4(x):
    return pltpu.roll(x, 4, 1)


def expert_kernel(
    got_ref, gate_hbm, up_hbm, down_hbm, out_hbm,
    gate_ref, up_ref, down_ref, rows_ref, hidden_ref, out_ref, in_sem, sem,
):
    width = 2 * got_ref.shape[2]
    half = width // 2
    hid = gate_ref.shape[0]
    full = EX * MAIN
    quarter = half // 2
    cuts = [(c, min(CUTS[i + 1], hid) - c) for i, c in enumerate(CUTS[:-1])]
    loads = []
    for c, n in cuts:
        cut = pl.ds(c, n)
        loads.append([(gate_hbm.at[cut], gate_ref.at[cut]), (up_hbm.at[cut], up_ref.at[cut])])
    loads.append([(down_hbm, down_ref)])
    count = 0
    for i, group in enumerate(loads):
        for j, (source, target) in enumerate(group):
            group[j] = pltpu.make_async_copy(source, target, in_sem.at[count])
            count += 1

    for group in loads:
        for copy in group:
            copy.start()
    rows_ref[0:full, 0:half] = got_ref[:, 0:MAIN, :].reshape(full, half)
    rows_ref[0:full, half:width] = got_ref[:, MAIN : 2 * MAIN, :].reshape(full, half)
    step = 256
    low = lax.broadcasted_iota(jnp.int32, (EX // 2, 8, step), 1) < REST
    for c in range(0, half, step):
        rest = got_ref[:, 2 * MAIN : BLK, c : c + step].astype(f32).reshape(EX // 2, 2, 8, step)
        even, odd = rest[:, 0], rest[:, 1]
        lo = jnp.where(low, even, swap4(odd))
        hi = jnp.where(low, swap4(even), odd)
        rows_ref[full:, c : c + step] = lo.reshape(EX * REST, step).astype(bf16)
        rows_ref[full:, half + c : half + c + step] = hi.reshape(EX * REST, step).astype(bf16)
    for (c, n), group in zip(cuts, loads):
        for copy in group:
            copy.wait()
        gate = dot_t(rows_ref[...], gate_ref[c : c + n, :])
        up = dot_t(rows_ref[...], up_ref[c : c + n, :])
        gate = 0.5 * gate
        hidden_ref[:, c : c + n] = ((gate + gate * jnp.tanh(gate)) * up).astype(bf16)
    loads[-1][0].wait()
    low = lax.broadcasted_iota(jnp.int32, (EX // 2, 8, quarter), 1) < REST
    sends = []

    def send(t, first, count):
        rows = pl.ds(first, count)
        copy = pltpu.make_async_copy(
            out_ref.at[:, t, rows, :], out_hbm.at[:, t, rows, :], sem.at[len(sends)]
        )
        copy.start()
        sends.append(copy)

    for t in range(2):
        rests = []
        for h in range(2):
            at = t * half + h * quarter
            part = dot(hidden_ref[...], down_ref[:, at : at + quarter])
            out_ref[:, t, h * MAIN : (h + 1) * MAIN, :] = (
                part[0:full].astype(bf16).reshape(EX, MAIN, quarter)
            )
            if h == 0:
                send(t, 0, MAIN)
            rests.append(part[full:].reshape(EX // 2, 8, quarter))
        lo, hi = rests
        even = jnp.where(low, lo, swap4(hi))
        odd = jnp.where(low, swap4(lo), hi)
        joined = jnp.stack([even, odd], axis=1).reshape(EX, 8, quarter)
        out_ref[:, t, 2 * MAIN : BLK, :] = joined.astype(bf16)
        send(t, MAIN, BLK - MAIN)
    for copy in sends:
        copy.wait()


def combine_kernel(back_ref, main_ref, rest_ref, base_ref, out_ref):
    quarter = back_ref.shape[3]
    lane = lax.broadcasted_iota(jnp.int32, rest_ref.shape, 1)
    for h in range(2):
        mine = (lane % (2 * REST) < REST) == (h == 0)
        few = jnp.where(mine, rest_ref[...].astype(f32), 0.0).astype(bf16)
        total = None
        for t in range(2):
            rows = back_ref[:, t, h * MAIN : (h + 1) * MAIN, :].reshape(EX * MAIN, quarter)
            part = dot(main_ref[...], rows)
            rest = back_ref[:, t, 2 * MAIN : BLK, :].reshape(EX * 2 * REST, quarter)
            part = part + dot(few, rest)
            total = part if total is None else total + part
        cols = slice(h * quarter, (h + 1) * quarter)
        out_ref[:, cols] = (base_ref[:, cols] + total).astype(bf16)


def call(body, out_shape, **kw):
    mib = kw.pop("mib", 16)
    return pl.pallas_call(
        body, out_shape=out_shape, compiler_params=pltpu.CompilerParams(vmem_limit_bytes=mib << 20), **kw
    )


vmem = pl.BlockSpec(memory_space=pltpu.VMEM)
smem = pl.BlockSpec(memory_space=pltpu.SMEM)
hbm = pl.BlockSpec(memory_space=pl.ANY)


def in_hbm(x):
    return pltpu.with_memory_space_constraint(x, pltpu.HBM)


def in_vmem(x):
    return pltpu.with_memory_space_constraint(x, pltpu.VMEM)


def per_device(
    tokens, norm_gain, router, expert_ids, modality,
    expert_gate, expert_up, expert_down, shared_gate, shared_up, shared_down,
):
    sds = jax.ShapeDtypeStruct
    width = tokens.shape[1]
    half = width // 2
    side = lax.axis_index("tensor").astype(jnp.int32).reshape(1)
    gain = norm_gain.reshape(1, width)
    flags = modality.reshape(1, TK)
    swap = [(0, 1), (1, 0)]
    other_tokens = lax.ppermute(tokens, "dp", swap)
    other_flags = lax.ppermute(flags, "dp", swap)

    outgoing = call(
        place_kernel,
        pltpu.HBM((EX, BLK, half), bf16),
        in_specs=[hbm] * 3,
        out_specs=hbm,
        scratch_shapes=[
            pltpu.VMEM((TK, width), bf16),
            pltpu.VMEM((1, width), f32),
            pltpu.VMEM((expert_ids.shape[1], TK), jnp.int32),
            pltpu.VMEM((EX, BLK, half), bf16),
            pltpu.SemaphoreType.DMA((3,)),
            pltpu.SemaphoreType.DMA((4,)),
        ],
        name="place",
    )(in_hbm(tokens), in_hbm(gain), in_hbm(expert_ids.T))
    got = lax.all_to_all(outgoing, "expert", 0, 0, tiled=True)

    hid = expert_gate.shape[2]
    piece = pltpu.HBM((TK, half), bf16)
    hidden = pltpu.VMEM((2, TK, shared_gate.shape[2]), bf16)
    part = pltpu.VMEM(shared_down.shape, bf16)
    main, rest, own, pair, *weights = call(
        weigh_kernel,
        (
            sds((TK, EX * MAIN), bf16),
            sds((TK, EX * 2 * REST), bf16),
            pltpu.HBM((TK, half), f32),
            piece,
            part,
            part,
            part,
        ),
        in_specs=[smem] + [vmem] * 5 + [hbm] * 3,
        scratch_shapes=[hidden, pltpu.SemaphoreType.DMA((3,))],
        name="weigh",
    )(
        side, tokens, gain, expert_ids.T, router.T, flags,
        in_hbm(shared_gate.swapaxes(1, 2)), in_hbm(shared_up.swapaxes(1, 2)), in_hbm(shared_down),
    )
    four = ("dp", "tensor")
    pair = lax.ppermute(pair, four, [(i, i ^ 1) for i in range(4)])
    near, far = call(
        shared_kernel,
        (piece, piece),
        in_specs=[smem] + [vmem] * 6,
        scratch_shapes=[hidden],
        name="shared",
    )(side, other_tokens, gain, other_flags, *[in_vmem(x) for x in weights])
    near = lax.ppermute(near, four, [(i, i ^ 2) for i in range(4)])
    far = lax.ppermute(far, four, [(i, i ^ 3) for i in range(4)])
    got, main, rest, own, pair, near, far = lax.optimization_barrier(
        (got, main, rest, own, pair, near, far)
    )
    base = own + pair.astype(f32) + near.astype(f32) + far.astype(f32)

    hid = expert_gate.shape[2]
    rows = EX * (MAIN + REST)
    results = call(
        expert_kernel,
        pltpu.HBM((EX, 2, BLK, half // 2), bf16),
        in_specs=[vmem, hbm, hbm, hbm],
        out_specs=hbm,
        scratch_shapes=[
            pltpu.VMEM((hid, width), bf16),
            pltpu.VMEM((hid, width), bf16),
            pltpu.VMEM((hid, width), bf16),
            pltpu.VMEM((rows, width), bf16),
            pltpu.VMEM((rows, hid), bf16),
            pltpu.VMEM((EX, 2, BLK, half // 2), bf16),
            pltpu.SemaphoreType.DMA((2 * len(CUTS) - 1,)),
            pltpu.SemaphoreType.DMA((4,)),
        ],
        mib=32,
        name="expert",
    )(got, in_hbm(expert_gate[0].T), in_hbm(expert_up[0].T), in_hbm(expert_down[0]))
    back = lax.all_to_all(
        results.reshape(2 * EX, BLK, half // 2), ("expert", "tensor"), 0, 0, tiled=True
    ).reshape(EX, 2, BLK, half // 2)
    return call(combine_kernel, sds((TK, half), bf16), name="combine")(back, main, rest, base)


def solution(mesh):
    in_specs = (
        P(("dp", "expert"), None),
        P(),
        P(),
        P(("dp", "expert"), None),
        P(("dp", "expert")),
        P("expert", None, "tensor"),
        P("expert", None, "tensor"),
        P("expert", "tensor", None),
        P(None, None, ("dp", "tensor")),
        P(None, None, ("dp", "tensor")),
        P(None, ("dp", "tensor"), None),
    )
    out_specs = P(("dp", "expert"), "tensor")
    return jax.shard_map(
        per_device, mesh=mesh, in_specs=in_specs, out_specs=out_specs, check_vma=False
    )
```
